128 devices in a mesh: chord: 8 (over y_lo, z), span: 16 (over x, y_hi, core).
Axes of the slice: x: 4, y: 4 (y_hi: 2, y_lo: 2; y = y_hi * 2 + y_lo), z: 4, core: 2. Of those that a mesh axis runs over, the one named last changes fastest.
Arguments:
- state: float32 [5, 125, 32, 32, 128], P(None, None, 'chord', 'span'), may hold values from -10 to 10
Outputs:
- residual: float32 [5, 125, 32, 32, 128], P(None, None, 'chord', 'span')
- viscosity: float32 [125, 32, 32, 128], P(None, 'chord', 'span')
The draws below stay inside these ranges and needn't reach their ends.
All inputs are finite; a program needn't handle non-finite values.
Results may differ from the reference program's by a relative error of at most 0.0001.
Values sent between devices are 32-bit elements; how exact they have to be, the bound alone decides.
A program may use at most 128 MiB of HBM per device.

```python
import math
import jax
import jax.numpy as jnp
import numpy as np
from jax import lax

NVAR = 5
NPTS = 125
NORMAL_ELEMENTS = 128
CHORD_ELEMENTS = 32
SPAN_ELEMENTS = 32


def draw_state(key, part):
    element_lattice = (CHORD_ELEMENTS, SPAN_ELEMENTS, NORMAL_ELEMENTS)
    variable = jnp.arange(NVAR).reshape(NVAR, 1, 1, 1, 1)
    level_base = jax.random.normal(jax.random.fold_in(key, 1), (NVAR, 1) + element_lattice, jnp.float32)
    density_base = jax.random.uniform(jax.random.fold_in(key, 2), (NVAR, 1) + element_lattice, jnp.float32, 0.5, 1.5)
    base = jnp.where(variable == 0, density_base, level_base)
    log_amp = jax.random.uniform(jax.random.fold_in(key, 3), (NVAR, 1) + element_lattice, jnp.float32, math.log(0.001), math.log(1.0))
    noise = jax.random.normal(jax.random.fold_in(key, 4), (NVAR, NPTS) + element_lattice, jnp.float32)
    return jnp.clip(base + jnp.exp(log_amp) * noise, -10.0, 10.0)


def setup_inputs(seed: int = 0) -> dict:
    key_of = jax.random.split(jax.random.key(seed), 2)
    return {
        "state": draw_state(jax.random.fold_in(key_of[1], 71), 0),
    }


EPS_SCALE = 0.01
SENSOR_CENTRE = -3.0
SENSOR_WIDTH = 1.5
RATIO_FLOOR = 1e-06
ENERGY_EPS = 1e-06
GAUSS_NODES = [-0.906179845938664, -0.5384693101056831, 0.0, 0.5384693101056831, 0.906179845938664]
GAUSS_WEIGHTS = [0.2369268850561891, 0.4786286704993665, 0.5688888888888889, 0.4786286704993665, 0.2369268850561891]

def legendre_values(points):
    values = [np.ones(points.shape), np.array(points)]
    for order in range(1, 5):
        values.append(((2 * order + 1) * points * values[order] - order * values[order - 1]) / (order + 1))
    return values

def line_tables():
    line_nodes = np.array(GAUSS_NODES)
    quadrature_weights = np.array(GAUSS_WEIGHTS)
    barycentric = np.array([1.0 / np.prod([line_nodes[j] - line_nodes[k] for k in range(5) if k != j]) for j in range(5)])
    derivative = np.zeros((5, 5))
    for i in range(5):
        for j in range(5):
            if i != j:
                derivative[i, j] = barycentric[j] / barycentric[i] / (line_nodes[i] - line_nodes[j])
        derivative[i, i] = -np.sum(derivative[i])
    left_values = np.ones(5)
    right_values = np.ones(5)
    for j in range(5):
        for k in range(5):
            if k != j:
                left_values[j] *= (-1.0 - line_nodes[k]) / (line_nodes[j] - line_nodes[k])
                right_values[j] *= (1.0 - line_nodes[k]) / (line_nodes[j] - line_nodes[k])
    legendre = legendre_values(line_nodes)
    fourth_slope = 7.0 * legendre[3] + 3.0 * legendre[1]
    fifth_slope = 9.0 * legendre[4] + 5.0 * legendre[2] + legendre[0]
    left_corr = 0.5 * (fourth_slope - fifth_slope)
    right_corr = 0.5 * (fourth_slope + fifth_slope)
    modal = np.zeros((5, 5))
    for k in range(5):
        modal[k, :] = quadrature_weights * math.sqrt((2 * k + 1) / 2.0) * legendre[k]
    return (line_nodes, derivative, left_values, right_values, left_corr, right_corr, modal)

def along_axis(operator_matrix, axis):
    factors = [np.eye(5), np.eye(5), np.eye(5)]
    factors[axis] = operator_matrix
    return np.kron(np.kron(factors[0], factors[1]), factors[2])

def build_tables():
    line_nodes, derivative, left_values, right_values, left_corr, right_corr, modal = line_tables()
    operators = []
    for axis in range(3):
        group = (along_axis(derivative, axis), along_axis(left_values[None, :], axis), along_axis(right_values[None, :], axis), along_axis(left_corr[:, None], axis), along_axis(right_corr[:, None], axis))
        operators.append(tuple((jnp.asarray(entry, dtype=jnp.float32) for entry in group)))
    modal_3d = jnp.asarray(np.kron(np.kron(modal, modal), modal), dtype=jnp.float32)
    point_index = np.arange(125)
    high_np = np.where((point_index // 25 == 4) | (point_index // 5 % 5 == 4) | (point_index % 5 == 4), 1.0, 0.0)
    high_mask = jnp.asarray(high_np, dtype=jnp.float32)
    halves = [(1.0 - line_nodes) / 2.0, (1.0 + line_nodes) / 2.0]
    trilinear_np = np.zeros((125, 8))
    for corner in range(8):
        trilinear_np[:, corner] = np.kron(np.kron(halves[corner // 4], halves[corner // 2 % 2]), halves[corner % 2])
    trilinear = jnp.asarray(trilinear_np, dtype=jnp.float32)
    return (operators, modal_3d, high_mask, trilinear)

def single_points(operator_matrix, field):
    return jnp.einsum('qp,pxyz->qxyz', operator_matrix, field, precision=lax.Precision.HIGHEST)

def sensor_viscosity(density, modal_3d, high_mask):
    coeffs = single_points(modal_3d, density)
    energy = coeffs * coeffs
    high_part = lax.optimization_barrier(jnp.sum(energy * high_mask[:, None, None, None], axis=0))
    total = lax.optimization_barrier(jnp.sum(energy, axis=0)) + ENERGY_EPS
    level = jnp.log10(jnp.maximum(high_part / total, RATIO_FLOOR))
    ramp = jnp.clip((level - SENSOR_CENTRE) / SENSOR_WIDTH, -1.0, 1.0)
    return EPS_SCALE * 0.5 * (1.0 + jnp.sin(0.5 * math.pi * ramp))

def boundary_masks(length, dim, rank, is_first, is_last):
    shape = [1] * rank
    shape[dim] = length
    place = lax.broadcasted_iota(jnp.int32, tuple(shape), dim)
    lower_open = jnp.logical_or(place > 0, jnp.logical_not(is_first))
    upper_open = jnp.logical_or(place < length - 1, jnp.logical_not(is_last))
    return (lower_open.astype(jnp.float32), upper_open.astype(jnp.float32))

def variable_residual(field, viscosity, operators):
    total = jnp.zeros_like(field)
    for axis in range(3):
        derivative, to_left, to_right, lift_left, lift_right = operators[axis]
        dim = axis + 1
        closed = axis != 1
        lower_open, upper_open = boundary_masks(field.shape[dim], dim, 4, closed, closed)
        left_tr = single_points(to_left, field)
        right_tr = single_points(to_right, field)
        prev_right = jnp.roll(right_tr, 1, axis=dim)
        following_left = jnp.roll(left_tr, -1, axis=dim)
        gradient = single_points(derivative, field) + single_points(lift_left, 0.5 * (prev_right - left_tr) * lower_open) + single_points(lift_right, 0.5 * (following_left - right_tr) * upper_open)
        flux = viscosity * gradient
        flux_left = single_points(to_left, flux)
        flux_right = single_points(to_right, flux)
        flux_prev = jnp.roll(flux_right, 1, axis=dim)
        flux_next = jnp.roll(flux_left, -1, axis=dim)
        total = total + single_points(derivative, flux) + single_points(lift_left, 0.5 * (flux_prev + flux_left) * lower_open - flux_left) + single_points(lift_right, 0.5 * (flux_next + flux_right) * upper_open - flux_right)
    return total

def reference(state):
    operators, modal_3d, high_mask, trilinear = build_tables()
    element_eps = sensor_viscosity(state[0], modal_3d, high_mask)
    padded = jnp.pad(element_eps, ((1, 1), (0, 0), (1, 1)))
    along_chord = jnp.maximum(padded[:-1], padded[1:])
    along_span = jnp.maximum(along_chord, jnp.roll(along_chord, 1, axis=1))
    vertex = jnp.maximum(along_span[:, :, :-1], along_span[:, :, 1:])
    shifted = jnp.roll(vertex, -1, axis=1)
    chord_count = element_eps.shape[0]
    normal_count = element_eps.shape[2]
    corner_list = []
    for corner in range(8):
        step_x = corner // 4
        step_y = corner // 2 % 2
        step_z = corner % 2
        source = shifted if step_y == 1 else vertex
        corner_list.append(source[step_x:step_x + chord_count, :, step_z:step_z + normal_count])
    corners = jnp.stack(corner_list, axis=0)
    viscosity = jnp.einsum('qc,cxyz->qxyz', trilinear, corners, precision=lax.Precision.HIGHEST)

    def one_variable(field):
        return variable_residual(field, viscosity, operators)
    residual = lax.map(one_variable, state)
    return (residual, viscosity)
```

```python
import functools
import math

import jax
import jax.numpy as jnp
import numpy as np
from jax import lax
from jax.experimental import pallas as pl
from jax.experimental.pallas import tpu as pltpu
from jax.sharding import PartitionSpec as P

MESH = pl.DeviceIdType.MESH
EPS_SCALE = 0.01
SENSOR_CENTRE = -3.0
SENSOR_WIDTH = 1.5
RATIO_FLOOR = 1e-06
ENERGY_EPS = 1e-06
NODES = [-0.906179845938664, -0.5384693101056831, 0.0, 0.5384693101056831, 0.906179845938664]
WEIGHTS = [
    0.2369268850561891,
    0.4786286704993665,
    0.5688888888888889,
    0.4786286704993665,
    0.2369268850561891,
]


def legendre_values(points):
    values = [np.ones(points.shape), np.array(points)]
    for order in range(1, 5):
        values.append(
            ((2 * order + 1) * points * values[order] - order * values[order - 1]) / (order + 1)
        )
    return values


def tables():
    x = np.array(NODES)
    w = np.array(WEIGHTS)
    bary = np.array([1.0 / np.prod([x[j] - x[k] for k in range(5) if k != j]) for j in range(5)])
    deriv = np.zeros((5, 5))
    for i in range(5):
        for j in range(5):
            if i != j:
                deriv[i, j] = bary[j] / bary[i] / (x[i] - x[j])
        deriv[i, i] = -np.sum(deriv[i])
    left = np.ones(5)
    right = np.ones(5)
    for j in range(5):
        for k in range(5):
            if k != j:
                left[j] *= (-1.0 - x[k]) / (x[j] - x[k])
                right[j] *= (1.0 - x[k]) / (x[j] - x[k])
    legendre = legendre_values(x)
    fourth = 7.0 * legendre[3] + 3.0 * legendre[1]
    fifth = 9.0 * legendre[4] + 5.0 * legendre[2] + legendre[0]
    half_l = 0.25 * (fourth - fifth)
    half_r = 0.25 * (fourth + fifth)
    modal = np.zeros((5, 5))
    for k in range(5):
        modal[k, :] = w * math.sqrt((2 * k + 1) / 2.0) * legendre[k]
    own = deriv - np.outer(half_l, left) - np.outer(half_r, right)
    upper = (1.0 + x) / 2.0
    near = float(np.sum(right * half_r * upper))
    far = float(np.sum(right * half_r * (1.0 - upper)))
    return own, left, right, half_l, half_r, modal, upper, near, far


OWN, LEFT, RIGHT, HALF_L, HALF_R, MODAL, UPPER, K_NEAR, K_FAR = tables()


def even_odd(u):
    return u[0] + u[4], u[1] + u[3], u[0] - u[4], u[1] - u[3], u[2]


def line_traces(eo):
    s0, s1, d0, d1, m = eo
    even = (
        float((RIGHT[0] + RIGHT[4]) / 2) * s0
        + float((RIGHT[1] + RIGHT[3]) / 2) * s1
        + float(RIGHT[2]) * m
    )
    odd = float((RIGHT[0] - RIGHT[4]) / 2) * d0 + float((RIGHT[1] - RIGHT[3]) / 2) * d1
    return even - odd, even + odd


def line_apply(eo, prev, following):
    s0, s1, d0, d1, m = eo
    sp = prev + following
    dp = prev - following
    out = [None] * 5
    for i in (0, 1):
        a = [(OWN[i, j] + OWN[i, 4 - j]) / 2 for j in (0, 1)]
        b = [(OWN[i, j] - OWN[i, 4 - j]) / 2 for j in (0, 1)]
        p = (
            float(a[0]) * s0
            + float(a[1]) * s1
            + float(OWN[i, 2]) * m
            + float((HALF_L[i] + HALF_R[i]) / 2) * sp
        )
        q = float(b[0]) * d0 + float(b[1]) * d1 + float((HALF_L[i] - HALF_R[i]) / 2) * dp
        out[i] = p + q
        out[4 - i] = q - p
    b = [(OWN[2, j] - OWN[2, 4 - j]) / 2 for j in (0, 1)]
    out[2] = float(b[0]) * d0 + float(b[1]) * d1 + float((HALF_L[2] - HALF_R[2]) / 2) * dp
    return out


def modal_line(u):
    s0, s1, d0, d1, m = even_odd(u)
    out = []
    for k in range(5):
        if k % 2 == 0:
            out.append(
                float(MODAL[k, 0]) * s0 + float(MODAL[k, 1]) * s1 + float(MODAL[k, 2]) * m
            )
        else:
            out.append(float(MODAL[k, 0]) * d0 + float(MODAL[k, 1]) * d1)
    return out


def rows_roll(x, shift):
    return pltpu.roll(x, shift % 8, axis=x.ndim - 2)


def lanes_roll(x, shift):
    return pltpu.roll(x, shift % 128, axis=x.ndim - 1)


GROUPS = ((0, 2), (2, 4), (4, 5))
PAIRS = 63
SPOTS = tuple((dc, ds) for dc in (-1, 0, 1) for ds in (-1, 0, 1) if (dc, ds) != (0, 0))


def kernel(
    chords,
    spans,
    x_hbm,
    res_hbm,
    vis_hbm,
    u,
    gs,
    gc,
    gn,
    r,
    vis,
    modes,
    ts,
    tc,
    tsf,
    usr,
    usl,
    ucu,
    ucd,
    vsr,
    vsl,
    vcu,
    vcd,
    fsr,
    fsl,
    fcu,
    fcd,
    hsr,
    hsl,
    hcu,
    hcd,
    eps,
    eps_in,
    ks,
    kc,
    load_sem,
    out_sem,
    e_send,
    e_recv,
    u_send,
    u_recv,
    f_send,
    f_recv,
):
    c = lax.axis_index("chord")
    s = lax.axis_index("span")
    has_lo = c > 0
    has_hi = c < chords - 1
    s_of = {0: s, 1: lax.rem(s + 1, spans), -1: lax.rem(s + spans - 1, spans)}
    c_of = {0: c, 1: lax.rem(c + 1, chords), -1: lax.rem(c + chords - 1, chords)}

    def exists(dc):
        return {0: None, 1: has_hi, -1: has_lo}[dc]

    def guarded(cond, action):
        if cond is None:
            action()
        else:
            pl.when(cond)(action)

    barrier = pltpu.get_barrier_semaphore()
    for dc, ds in SPOTS:
        guarded(
            exists(dc),
            lambda dc=dc, ds=ds: pl.semaphore_signal(
                barrier, inc=1, device_id=(c_of[dc], s_of[ds]), device_id_type=MESH
            ),
        )

    loads = [pltpu.make_async_copy(x_hbm.at[v], u.at[v], load_sem.at[v]) for v in range(5)]
    for copy in loads:
        copy.start()

    row = lax.broadcasted_iota(jnp.int32, (8, 128), 0)
    lane = lax.broadcasted_iota(jnp.int32, (8, 128), 1)
    low_j = lax.rem(row, 2) == 0
    row_lo = row < 2
    row_hi = row >= 6
    first_lane = lane == 0
    last_lane = lane == 127

    def pick(mask, a, b):
        if a.ndim == 3:
            mask = jnp.broadcast_to(mask[None], a.shape)
        return jnp.where(mask, a, b)

    loads[0].wait()

    def modes_cb(a, carry):
        block = u[0, pl.ds(25 * a, 25)].reshape(5, 5, 8, 128)
        along_c = modal_line([block[:, k] for k in range(5)])
        stacked = [jnp.stack([along_c[o][b] for o in range(5)]) for b in range(5)]
        along_b = modal_line(stacked)
        for n in range(5):
            modes[pl.ds(25 * a + 5 * n, 5)] = along_b[n]
        return carry

    lax.fori_loop(0, 5, modes_cb, 0)
    low = jnp.zeros((4, 8, 128), jnp.float32)
    high = jnp.zeros((8, 128), jnp.float32)
    high4 = jnp.zeros((5, 8, 128), jnp.float32)
    for n in range(5):
        along_a = modal_line([modes[25 * a + 5 * n : 25 * a + 5 * n + 5] for a in range(5)])
        for m in range(5):
            square = along_a[m] * along_a[m]
            if n == 4 or m == 4:
                high4 = high4 + square
            else:
                low = low + square[:4]
                high = high + square[4]
    high = high + (high4[0] + high4[1]) + (high4[2] + high4[3]) + high4[4]
    total = (low[0] + low[1]) + (low[2] + low[3]) + high
    ratio = high / (total + ENERGY_EPS)
    level = jnp.log(jnp.maximum(ratio, RATIO_FLOOR)) * (1.0 / math.log(10.0))
    ramp = jnp.clip((level - SENSOR_CENTRE) / SENSOR_WIDTH, -1.0, 1.0)
    eps[...] = (EPS_SCALE * 0.5) * (1.0 + jnp.sin((0.5 * math.pi) * ramp))

    for v in range(1, 5):
        loads[v].wait()

    def local_ab(k, carry):
        v = k // 5
        a = k - 5 * v
        block = u[v, pl.ds(25 * a, 25)].reshape(5, 5, 8, 128)
        eo = even_odd([block[b] for b in range(5)])
        tl, tr = line_traces(eo)
        ts[pl.ds(25 * v + 5 * a, 5)] = pick(low_j, tl, tr)
        zero = jnp.zeros_like(tl)
        grad = line_apply(
            eo, pick(low_j, zero, rows_roll(tr, 1)), pick(low_j, rows_roll(tl, -1), zero)
        )
        for b in range(5):
            gs[v, pl.ds(25 * a + 5 * b, 5)] = grad[b]
        eo = even_odd([block[:, k] for k in range(5)])
        tl, tr = line_traces(eo)
        grad = line_apply(
            eo,
            pick(first_lane, tl, lanes_roll(tr, 1)),
            pick(last_lane, tr, lanes_roll(tl, -1)),
        )
        for b in range(5):
            gn[v, pl.ds(25 * a + 5 * b, 5)] = jnp.stack([grad[k][b] for k in range(5)])
        return carry

    lax.fori_loop(0, 25, local_ab, 0)

    def local_c(k, carry):
        v = k // 5
        b = k - 5 * v
        eo = even_odd([u[v, pl.ds(25 * a + 5 * b, 5)] for a in range(5)])
        tl, tr = line_traces(eo)
        q = 25 * v + 5 * b
        tc[pl.ds(q, 5)] = pick(row_lo, tl, tr)
        ucu[pl.ds(q, 5)] = tr[:, 6:8]
        ucd[pl.ds(q, 5)] = tl[:, 0:2]
        zero = jnp.zeros_like(tl)
        grad = line_apply(
            eo, pick(row_lo, zero, rows_roll(tr, 2)), pick(row_hi, zero, rows_roll(tl, -2))
        )
        for a in range(5):
            gc[v, pl.ds(25 * a + 5 * b, 5)] = grad[a]
        return carry

    lax.fori_loop(0, 25, local_c, 0)
    ts[125] = jnp.zeros((8, 128), jnp.float32)
    tsf[125] = jnp.zeros((8, 128), jnp.float32)

    def pack(src, to_right, to_left, start, count):
        def body(k, carry):
            p = start + k * 1
            two = src[pl.ds(2 * p, 2)]
            to_right[p] = jnp.where(low_j, rows_roll(two[0], -1), two[1])
            to_left[p] = jnp.where(low_j, two[0], rows_roll(two[1], 1))
            return carry

        lax.fori_loop(0, count, body, 0)

    def unpack(from_left, from_right, p):
        a, b = from_left[p], from_right[p]
        return (
            jnp.where(low_j, a, rows_roll(b, 1)),
            jnp.where(low_j, rows_roll(a, -1), b),
        )

    pack(ts, usr, usl, 0, PAIRS)

    pl.semaphore_wait(barrier, 2 + jnp.where(has_lo, 3, 0) + jnp.where(has_hi, 3, 0))

    eps_copies = []
    for k, (dc, ds) in enumerate(SPOTS):
        copy = pltpu.make_async_remote_copy(
            src_ref=eps,
            dst_ref=eps_in.at[k],
            send_sem=e_send.at[k],
            recv_sem=e_recv.at[k],
            device_id=(c_of[dc], s_of[ds]),
            device_id_type=MESH,
        )
        guarded(exists(dc), copy.start)
        eps_copies.append((dc, ds, copy))

    def exchange(bufs, sems, g):
        (sr, sl, cu, cd), (dr, dl, du, dd) = bufs
        v0, v1 = GROUPS[g]
        pairs = pl.ds(25 * v0 // 2, -(-25 * (v1 - v0) // 2))
        lines = pl.ds(25 * v0, 25 * (v1 - v0))
        out = []
        for k, (src, dst, dc, ds, part) in enumerate(
            (
                (sr, dr, 0, 1, pairs),
                (sl, dl, 0, -1, pairs),
                (cu, du, 1, 0, lines),
                (cd, dd, -1, 0, lines),
            )
        ):
            copy = pltpu.make_async_remote_copy(
                src_ref=src.at[part],
                dst_ref=dst.at[part],
                send_sem=sems[0].at[4 * g + k],
                recv_sem=sems[1].at[4 * g + k],
                device_id=(c_of[dc], s_of[ds]),
                device_id_type=MESH,
            )
            out.append((dc, copy))
        return out

    u_copies = [
        exchange(((usr, usl, ucu, ucd), (vsr, vsl, vcu, vcd)), (u_send, u_recv), g)
        for g in range(3)
    ]
    f_copies = [
        exchange(((fsr, fsl, fcu, fcd), (hsr, hsl, hcu, hcd)), (f_send, f_recv), g)
        for g in range(3)
    ]

    def start(copies):
        for dc, copy in copies:
            guarded(exists(dc), copy.start)

    def arrive(copies):
        for dc, copy in copies:
            guarded(exists(-dc), copy.wait_recv)

    def sent(copies):
        for dc, copy in copies:
            guarded(exists(dc), copy.wait_send)

    for g in range(3):
        start(u_copies[g])

    for dc, ds, copy in eps_copies:
        guarded(exists(-dc), copy.wait_recv)

    around = {(0, 0): eps[...]}
    for k, (dc, ds) in enumerate(SPOTS):
        value = eps_in[k]
        cond = exists(-dc)
        if cond is not None:
            value = jnp.where(cond, value, jnp.zeros_like(value))
        around[(-dc, -ds)] = value
    faces = {}
    for dc in (-1, 0, 1):
        mid, left, right = around[(dc, 0)], around[(dc, -1)], around[(dc, 1)]
        before = jnp.where(low_j, rows_roll(left, -1), rows_roll(mid, 1))
        after = jnp.where(low_j, rows_roll(mid, -1), rows_roll(right, 1))
        beyond = jnp.where(low_j, left, right)
        faces[dc] = (
            jnp.maximum(before, mid),
            jnp.maximum(mid, after),
            jnp.maximum(beyond, jnp.where(low_j, before, after)),
        )

    def normal_pair(x):
        zero = jnp.zeros_like(x)
        return (
            jnp.maximum(x, jnp.where(first_lane, zero, lanes_roll(x, 1))),
            jnp.maximum(x, jnp.where(last_lane, zero, lanes_roll(x, -1))),
        )

    corner = {}
    span_far = {}
    chord_far = {}
    for k in range(3):
        below, mid, above = faces[-1][k], faces[0][k], faces[1][k]
        before = jnp.where(row_lo, rows_roll(below, 2), rows_roll(mid, 2))
        after = jnp.where(row_hi, rows_roll(above, -2), rows_roll(mid, -2))
        for sx, value in ((0, jnp.maximum(before, mid)), (1, jnp.maximum(mid, after))):
            pair = normal_pair(value)
            for sz in range(2):
                if k == 2:
                    span_far[(sx, sz)] = pair[sz]
                else:
                    corner[(sx, k, sz)] = pair[sz]
        if k < 2:
            beyond = jnp.where(row_lo, rows_roll(below, 4), rows_roll(above, 4))
            pair = normal_pair(jnp.maximum(beyond, jnp.where(row_lo, before, after)))
            for sz in range(2):
                chord_far[(k, sz)] = pair[sz]

    def between(lo, hi):
        step = hi - lo
        return [lo + float(UPPER[i]) * step for i in range(5)]

    plane = {
        (sy, sz): between(corner[(0, sy, sz)], corner[(1, sy, sz)])
        for sy in range(2)
        for sz in range(2)
    }
    for a in range(5):
        edge = [between(plane[(0, sz)][a], plane[(1, sz)][a]) for sz in range(2)]
        for b in range(5):
            vis[pl.ds(25 * a + 5 * b, 5)] = jnp.stack(between(edge[0][b], edge[1][b]))
    vis_copy = pltpu.make_async_copy(vis, vis_hbm, out_sem.at[5])
    vis_copy.start()
    weight = {}
    for sx in range(2):
        for sz in range(2):
            near = jnp.where(low_j, corner[(sx, 0, sz)], corner[(sx, 1, sz)])
            value = K_FAR * span_far[(sx, sz)] + K_NEAR * near
            weight[(sx, sz)] = jnp.where(low_j, value, -value)
    edge = [between(weight[(0, sz)], weight[(1, sz)]) for sz in range(2)]
    for a in range(5):
        ks[pl.ds(5 * a, 5)] = jnp.stack(between(edge[0][a], edge[1][a]))
    for sy in range(2):
        for sz in range(2):
            near = jnp.where(row_lo, corner[(0, sy, sz)], corner[(1, sy, sz)])
            value = K_FAR * chord_far[(sy, sz)] + K_NEAR * near
            weight[(sy, sz)] = jnp.where(row_lo, value, -value)
    edge = [between(weight[(0, sz)], weight[(1, sz)]) for sz in range(2)]
    for b in range(5):
        kc[pl.ds(5 * b, 5)] = jnp.stack(between(edge[0][b], edge[1][b]))

    span_trace = [jnp.where(low_j, float(LEFT[b]), float(RIGHT[b])) for b in range(5)]
    chord_trace = [jnp.where(row_lo, float(LEFT[a]), float(RIGHT[a])) for a in range(5)]
    span_lift = [jnp.where(low_j, float(HALF_L[b]), float(HALF_R[b])) for b in range(5)]
    chord_lift = [
        jnp.where(row_lo, float(HALF_L[a]), jnp.where(row_hi, float(HALF_R[a]), 0.0))
        for a in range(5)
    ]

    def flux_traces(k, carry):
        v = k // 5
        a = k - 5 * v
        at = [pl.ds(25 * a + 5 * b, 5) for b in range(5)]
        acc = None
        for b in range(5):
            term = span_trace[b][None] * (vis[at[b]] * gs[v, at[b]])
            acc = term if acc is None else acc + term
        tsf[pl.ds(25 * v + 5 * a, 5)] = acc
        at = [pl.ds(25 * i + 5 * a, 5) for i in range(5)]
        acc = None
        for i in range(5):
            term = chord_trace[i][None] * (vis[at[i]] * gc[v, at[i]])
            acc = term if acc is None else acc + term
        q = 25 * v + 5 * a
        fcu[pl.ds(q, 5)] = acc[:, 6:8]
        fcd[pl.ds(q, 5)] = acc[:, 0:2]
        return carry

    for g, (v0, v1) in enumerate(GROUPS):
        lax.fori_loop(5 * v0, 5 * v1, flux_traces, 0)
        pack(tsf, fsr, fsl, 25 * v0 // 2, -(-25 * (v1 - v0) // 2))
        start(f_copies[g])

    def normal_part(k, carry):
        v = k // 5
        a = k - 5 * v
        block = gn[v, pl.ds(25 * a, 25)] * vis[pl.ds(25 * a, 25)]
        block = block.reshape(5, 5, 8, 128)
        eo = even_odd([block[:, i] for i in range(5)])
        tl, tr = line_traces(eo)
        out = line_apply(
            eo,
            pick(first_lane, -tl, lanes_roll(tr, 1)),
            pick(last_lane, -tr, lanes_roll(tl, -1)),
        )
        for b in range(5):
            r[v, pl.ds(25 * a + 5 * b, 5)] = jnp.stack([out[i][b] for i in range(5)])
        return carry

    lax.fori_loop(0, 25, normal_part, 0)

    end_lo = jnp.logical_and(row_lo, jnp.logical_not(has_lo))
    end_hi = jnp.logical_and(row_hi, jnp.logical_not(has_hi))

    def unpack_all(from_left, from_right, dst, start_pair, count):
        def body(k, carry):
            p = start_pair + k
            first, second = unpack(from_left, from_right, p)
            dst[2 * p] = first
            dst[2 * p + 1] = second
            return carry

        lax.fori_loop(0, count, body, 0)

    def chord_outer(from_lo, from_hi, q):
        lo = from_lo[pl.ds(q, 5)]
        hi = from_hi[pl.ds(q, 5)]
        gap = jnp.zeros((5, 4, 128), jnp.float32)
        return jnp.concatenate([lo, gap, hi], axis=1)

    def span_part(k, carry):
        v = k // 5
        a = k - 5 * v
        outer = tsf[pl.ds(25 * v + 5 * a, 5)]
        flux = [
            vis[pl.ds(25 * a + 5 * b, 5)]
            * (gs[v, pl.ds(25 * a + 5 * b, 5)] + span_lift[b][None] * outer)
            for b in range(5)
        ]
        eo = even_odd(flux)
        tl, tr = line_traces(eo)
        zero = jnp.zeros_like(tl)
        out = line_apply(
            eo, pick(low_j, zero, rows_roll(tr, 1)), pick(low_j, rows_roll(tl, -1), zero)
        )
        for b in range(5):
            at = pl.ds(25 * a + 5 * b, 5)
            r[v, at] = r[v, at] + out[b]
        return carry

    def chord_part(k, carry):
        v = k // 5
        b = k - 5 * v
        q = 25 * v + 5 * b
        own = tc[pl.ds(q, 5)]
        outer = chord_outer(vcu, vcd, q)
        outer = pick(jnp.logical_or(end_lo, end_hi), own, outer)
        flux = [
            vis[pl.ds(25 * a + 5 * b, 5)]
            * (gc[v, pl.ds(25 * a + 5 * b, 5)] + chord_lift[a][None] * outer)
            for a in range(5)
        ]
        eo = even_odd(flux)
        tl, tr = line_traces(eo)
        zero = jnp.zeros_like(tl)
        out = line_apply(
            eo,
            pick(row_lo, pick(end_lo, -tl, zero), rows_roll(tr, 2)),
            pick(row_hi, pick(end_hi, -tr, zero), rows_roll(tl, -2)),
        )
        for a in range(5):
            at = pl.ds(25 * a + 5 * b, 5)
            r[v, at] = r[v, at] + out[a]
        return carry

    for g, (v0, v1) in enumerate(GROUPS):
        arrive(u_copies[g])
        unpack_all(vsr, vsl, tsf, 25 * v0 // 2, -(-25 * (v1 - v0) // 2))
        lax.fori_loop(5 * v0, 5 * v1, span_part, 0)
        lax.fori_loop(5 * v0, 5 * v1, chord_part, 0)

    def finish(k, carry):
        v = k // 5
        a = k - 5 * v
        q = 25 * v + 5 * a
        outer = tsf[pl.ds(q, 5)] + ks[pl.ds(5 * a, 5)] * ts[pl.ds(q, 5)]
        for b in range(5):
            at = pl.ds(25 * a + 5 * b, 5)
            r[v, at] = r[v, at] + span_lift[b][None] * outer
        return carry

    def finish_chord(k, carry):
        v = k // 5
        b = k - 5 * v
        q = 25 * v + 5 * b
        outer = chord_outer(hcu, hcd, q) + kc[pl.ds(5 * b, 5)] * tc[pl.ds(q, 5)]
        outer = pick(jnp.logical_or(end_lo, end_hi), jnp.zeros_like(outer), outer)
        for a in range(5):
            at = pl.ds(25 * a + 5 * b, 5)
            r[v, at] = r[v, at] + chord_lift[a][None] * outer
        return carry

    outs = [vis_copy]
    for g, (v0, v1) in enumerate(GROUPS):
        arrive(f_copies[g])
        unpack_all(hsr, hsl, tsf, 25 * v0 // 2, -(-25 * (v1 - v0) // 2))
        lax.fori_loop(5 * v0, 5 * v1, finish, 0)
        lax.fori_loop(5 * v0, 5 * v1, finish_chord, 0)
        copy = pltpu.make_async_copy(
            r.at[pl.ds(v0, v1 - v0)], res_hbm.at[pl.ds(v0, v1 - v0)], out_sem.at[g]
        )
        copy.start()
        outs.append(copy)
    for dc, ds, copy in eps_copies:
        guarded(exists(dc), copy.wait_send)
    for g in range(3):
        sent(u_copies[g])
        sent(f_copies[g])
    for copy in outs:
        copy.wait()


def shards(state):
    chords, spans = lax.axis_size("chord"), lax.axis_size("span")
    f32 = jnp.float32
    field = pltpu.VMEM((5, 125, 8, 128), f32)
    pairs = pltpu.VMEM((PAIRS, 8, 128), f32)
    thin = pltpu.VMEM((132, 2, 128), f32)
    sem = pltpu.SemaphoreType.DMA
    residual, viscosity = pl.pallas_call(
        functools.partial(kernel, chords, spans),
        out_shape=(
            jax.ShapeDtypeStruct((5, 125, 8, 128), f32),
            jax.ShapeDtypeStruct((125, 8, 128), f32),
        ),
        in_specs=[pl.BlockSpec(memory_space=pl.ANY)],
        out_specs=(pl.BlockSpec(memory_space=pl.ANY), pl.BlockSpec(memory_space=pl.ANY)),
        scratch_shapes=[
            field,
            field,
            field,
            field,
            field,
            pltpu.VMEM((125, 8, 128), f32),
            pltpu.VMEM((125, 8, 128), f32),
            pltpu.VMEM((126, 8, 128), f32),
            pltpu.VMEM((125, 8, 128), f32),
            pltpu.VMEM((126, 8, 128), f32),
        ]
        + [pairs, pairs, thin, thin] * 4
        + [
            pltpu.VMEM((8, 128), f32),
            pltpu.VMEM((8, 8, 128), f32),
            pltpu.VMEM((25, 8, 128), f32),
            pltpu.VMEM((25, 8, 128), f32),
            sem((5,)),
            sem((6,)),
            sem((8,)),
            sem((8,)),
            sem((12,)),
            sem((12,)),
            sem((12,)),
            sem((12,)),
        ],
        compiler_params=pltpu.CompilerParams(
            collective_id=0, has_side_effects=True, vmem_limit_bytes=56 * 1024 * 1024
        ),
        name="viscous",
    )(state.reshape(5, 125, 8, 128))
    return residual.reshape(state.shape), viscosity.reshape(state.shape[1:])


def solution(mesh):
    in_specs = (P(None, None, "chord", "span", None),)
    out_specs = (P(None, None, "chord", "span", None), P(None, "chord", "span", None))
    return jax.shard_map(shards, mesh=mesh, in_specs=in_specs, out_specs=out_specs, check_vma=False)
```

```python
import functools
import math

import jax
import jax.numpy as jnp
import numpy as np
from jax import lax
from jax.experimental import pallas as pl
from jax.experimental.pallas import tpu as pltpu
from jax.sharding import PartitionSpec as P

MESH = pl.DeviceIdType.MESH
EPS_SCALE = 0.01
SENSOR_CENTRE = -3.0
SENSOR_WIDTH = 1.5
RATIO_FLOOR = 1e-06
ENERGY_EPS = 1e-06
NODES = [-0.906179845938664, -0.5384693101056831, 0.0, 0.5384693101056831, 0.906179845938664]
WEIGHTS = [
    0.2369268850561891,
    0.4786286704993665,
    0.5688888888888889,
    0.4786286704993665,
    0.2369268850561891,
]


def legendre_values(points):
    values = [np.ones(points.shape), np.array(points)]
    for order in range(1, 5):
        values.append(
            ((2 * order + 1) * points * values[order] - order * values[order - 1]) / (order + 1)
        )
    return values


def tables():
    x = np.array(NODES)
    w = np.array(WEIGHTS)
    bary = np.array([1.0 / np.prod([x[j] - x[k] for k in range(5) if k != j]) for j in range(5)])
    deriv = np.zeros((5, 5))
    for i in range(5):
        for j in range(5):
            if i != j:
                deriv[i, j] = bary[j] / bary[i] / (x[i] - x[j])
        deriv[i, i] = -np.sum(deriv[i])
    left = np.ones(5)
    right = np.ones(5)
    for j in range(5):
        for k in range(5):
            if k != j:
                left[j] *= (-1.0 - x[k]) / (x[j] - x[k])
                right[j] *= (1.0 - x[k]) / (x[j] - x[k])
    legendre = legendre_values(x)
    fourth = 7.0 * legendre[3] + 3.0 * legendre[1]
    fifth = 9.0 * legendre[4] + 5.0 * legendre[2] + legendre[0]
    half_l = 0.25 * (fourth - fifth)
    half_r = 0.25 * (fourth + fifth)
    modal = np.zeros((5, 5))
    for k in range(5):
        modal[k, :] = w * math.sqrt((2 * k + 1) / 2.0) * legendre[k]
    own = deriv - np.outer(half_l, left) - np.outer(half_r, right)
    upper = (1.0 + x) / 2.0
    near = float(np.sum(right * half_r * upper))
    far = float(np.sum(right * half_r * (1.0 - upper)))
    return own, left, right, half_l, half_r, modal, upper, near, far


OWN, LEFT, RIGHT, HALF_L, HALF_R, MODAL, UPPER, K_NEAR, K_FAR = tables()


def even_odd(u):
    return u[0] + u[4], u[1] + u[3], u[0] - u[4], u[1] - u[3], u[2]


def line_traces(eo):
    s0, s1, d0, d1, m = eo
    even = (
        float((RIGHT[0] + RIGHT[4]) / 2) * s0
        + float((RIGHT[1] + RIGHT[3]) / 2) * s1
        + float(RIGHT[2]) * m
    )
    odd = float((RIGHT[0] - RIGHT[4]) / 2) * d0 + float((RIGHT[1] - RIGHT[3]) / 2) * d1
    return even - odd, even + odd


def line_apply(eo, prev, following):
    s0, s1, d0, d1, m = eo
    sp = prev + following
    dp = prev - following
    out = [None] * 5
    for i in (0, 1):
        a = [(OWN[i, j] + OWN[i, 4 - j]) / 2 for j in (0, 1)]
        b = [(OWN[i, j] - OWN[i, 4 - j]) / 2 for j in (0, 1)]
        p = (
            float(a[0]) * s0
            + float(a[1]) * s1
            + float(OWN[i, 2]) * m
            + float((HALF_L[i] + HALF_R[i]) / 2) * sp
        )
        q = float(b[0]) * d0 + float(b[1]) * d1 + float((HALF_L[i] - HALF_R[i]) / 2) * dp
        out[i] = p + q
        out[4 - i] = q - p
    b = [(OWN[2, j] - OWN[2, 4 - j]) / 2 for j in (0, 1)]
    out[2] = float(b[0]) * d0 + float(b[1]) * d1 + float((HALF_L[2] - HALF_R[2]) / 2) * dp
    return out


def modal_line(u):
    s0, s1, d0, d1, m = even_odd(u)
    out = []
    for k in range(5):
        if k % 2 == 0:
            out.append(
                float(MODAL[k, 0]) * s0 + float(MODAL[k, 1]) * s1 + float(MODAL[k, 2]) * m
            )
        else:
            out.append(float(MODAL[k, 0]) * d0 + float(MODAL[k, 1]) * d1)
    return out


def rows_roll(x, shift):
    return pltpu.roll(x, shift % 8, axis=x.ndim - 2)


def lanes_roll(x, shift):
    return pltpu.roll(x, shift % 128, axis=x.ndim - 1)


GROUPS = ((0, 2), (2, 4), (4, 5))
PAIRS = 63
SPOTS = tuple((dc, ds) for dc in (-1, 0, 1) for ds in (-1, 0, 1) if (dc, ds) != (0, 0))


def kernel(
    chords,
    spans,
    x_hbm,
    r,
    vis,
    u,
    gs,
    gc,
    gn,
    modes,
    ts,
    tc,
    tsf,
    usr,
    usl,
    ucu,
    ucd,
    vsr,
    vsl,
    vcu,
    vcd,
    fsr,
    fsl,
    fcu,
    fcd,
    hsr,
    hsl,
    hcu,
    hcd,
    eps,
    eps_in,
    ks,
    kc,
    load_sem,
    e_send,
    e_recv,
    u_send,
    u_recv,
    f_send,
    f_recv,
):
    c = lax.axis_index("chord")
    s = lax.axis_index("span")
    has_lo = c > 0
    has_hi = c < chords - 1
    s_of = {0: s, 1: lax.rem(s + 1, spans), -1: lax.rem(s + spans - 1, spans)}
    c_of = {0: c, 1: lax.rem(c + 1, chords), -1: lax.rem(c + chords - 1, chords)}

    def exists(dc):
        return {0: None, 1: has_hi, -1: has_lo}[dc]

    def guarded(cond, action):
        if cond is None:
            action()
        else:
            pl.when(cond)(action)

    barrier = pltpu.get_barrier_semaphore()
    for dc, ds in SPOTS:
        guarded(
            exists(dc),
            lambda dc=dc, ds=ds: pl.semaphore_signal(
                barrier, inc=1, device_id=(c_of[dc], s_of[ds]), device_id_type=MESH
            ),
        )

    loads = [pltpu.make_async_copy(x_hbm.at[v], u.at[v], load_sem.at[v]) for v in range(5)]
    for copy in loads:
        copy.start()

    row = lax.broadcasted_iota(jnp.int32, (8, 128), 0)
    lane = lax.broadcasted_iota(jnp.int32, (8, 128), 1)
    low_j = lax.rem(row, 2) == 0
    row_lo = row < 2
    row_hi = row >= 6
    first_lane = lane == 0
    last_lane = lane == 127

    def pick(mask, a, b):
        if a.ndim == 3:
            mask = jnp.broadcast_to(mask[None], a.shape)
        return jnp.where(mask, a, b)

    loads[0].wait()

    def modes_cb(a, carry):
        block = u[0, pl.ds(25 * a, 25)].reshape(5, 5, 8, 128)
        along_c = modal_line([block[:, k] for k in range(5)])
        stacked = [jnp.stack([along_c[o][b] for o in range(5)]) for b in range(5)]
        along_b = modal_line(stacked)
        for n in range(5):
            modes[pl.ds(25 * a + 5 * n, 5)] = along_b[n]
        return carry

    lax.fori_loop(0, 5, modes_cb, 0)
    low = jnp.zeros((4, 8, 128), jnp.float32)
    high = jnp.zeros((8, 128), jnp.float32)
    high4 = jnp.zeros((5, 8, 128), jnp.float32)
    for n in range(5):
        along_a = modal_line([modes[25 * a + 5 * n : 25 * a + 5 * n + 5] for a in range(5)])
        for m in range(5):
            square = along_a[m] * along_a[m]
            if n == 4 or m == 4:
                high4 = high4 + square
            else:
                low = low + square[:4]
                high = high + square[4]
    high = high + (high4[0] + high4[1]) + (high4[2] + high4[3]) + high4[4]
    total = (low[0] + low[1]) + (low[2] + low[3]) + high
    ratio = high / (total + ENERGY_EPS)
    level = jnp.log(jnp.maximum(ratio, RATIO_FLOOR)) * (1.0 / math.log(10.0))
    ramp = jnp.clip((level - SENSOR_CENTRE) / SENSOR_WIDTH, -1.0, 1.0)
    eps[...] = (EPS_SCALE * 0.5) * (1.0 + jnp.sin((0.5 * math.pi) * ramp))

    for v in range(1, 5):
        loads[v].wait()

    def local_ab(k, carry):
        v = k // 5
        a = k - 5 * v
        block = u[v, pl.ds(25 * a, 25)].reshape(5, 5, 8, 128)
        eo = even_odd([block[b] for b in range(5)])
        tl, tr = line_traces(eo)
        ts[pl.ds(25 * v + 5 * a, 5)] = pick(low_j, tl, tr)
        zero = jnp.zeros_like(tl)
        grad = line_apply(
            eo, pick(low_j, zero, rows_roll(tr, 1)), pick(low_j, rows_roll(tl, -1), zero)
        )
        for b in range(5):
            gs[v, pl.ds(25 * a + 5 * b, 5)] = grad[b]
        eo = even_odd([block[:, k] for k in range(5)])
        tl, tr = line_traces(eo)
        grad = line_apply(
            eo,
            pick(first_lane, tl, lanes_roll(tr, 1)),
            pick(last_lane, tr, lanes_roll(tl, -1)),
        )
        for b in range(5):
            gn[v, pl.ds(25 * a + 5 * b, 5)] = jnp.stack([grad[k][b] for k in range(5)])
        return carry

    lax.fori_loop(0, 25, local_ab, 0)

    def local_c(k, carry):
        v = k // 5
        b = k - 5 * v
        eo = even_odd([u[v, pl.ds(25 * a + 5 * b, 5)] for a in range(5)])
        tl, tr = line_traces(eo)
        q = 25 * v + 5 * b
        tc[pl.ds(q, 5)] = pick(row_lo, tl, tr)
        ucu[pl.ds(q, 5)] = tr[:, 6:8]
        ucd[pl.ds(q, 5)] = tl[:, 0:2]
        zero = jnp.zeros_like(tl)
        grad = line_apply(
            eo, pick(row_lo, zero, rows_roll(tr, 2)), pick(row_hi, zero, rows_roll(tl, -2))
        )
        for a in range(5):
            gc[v, pl.ds(25 * a + 5 * b, 5)] = grad[a]
        return carry

    lax.fori_loop(0, 25, local_c, 0)
    ts[125] = jnp.zeros((8, 128), jnp.float32)
    tsf[125] = jnp.zeros((8, 128), jnp.float32)

    def pack(src, to_right, to_left, start, count):
        def body(k, carry):
            p = start + k * 1
            two = src[pl.ds(2 * p, 2)]
            to_right[p] = jnp.where(low_j, rows_roll(two[0], -1), two[1])
            to_left[p] = jnp.where(low_j, two[0], rows_roll(two[1], 1))
            return carry

        lax.fori_loop(0, count, body, 0)

    def unpack(from_left, from_right, p):
        a, b = from_left[p], from_right[p]
        return (
            jnp.where(low_j, a, rows_roll(b, 1)),
            jnp.where(low_j, rows_roll(a, -1), b),
        )

    pack(ts, usr, usl, 0, PAIRS)

    pl.semaphore_wait(barrier, 2 + jnp.where(has_lo, 3, 0) + jnp.where(has_hi, 3, 0))

    eps_copies = []
    for k, (dc, ds) in enumerate(SPOTS):
        copy = pltpu.make_async_remote_copy(
            src_ref=eps,
            dst_ref=eps_in.at[k],
            send_sem=e_send.at[k],
            recv_sem=e_recv.at[k],
            device_id=(c_of[dc], s_of[ds]),
            device_id_type=MESH,
        )
        guarded(exists(dc), copy.start)
        eps_copies.append((dc, ds, copy))

    def exchange(bufs, sems, g):
        (sr, sl, cu, cd), (dr, dl, du, dd) = bufs
        v0, v1 = GROUPS[g]
        pairs = pl.ds(25 * v0 // 2, -(-25 * (v1 - v0) // 2))
        lines = pl.ds(25 * v0, 25 * (v1 - v0))
        out = []
        for k, (src, dst, dc, ds, part) in enumerate(
            (
                (sr, dr, 0, 1, pairs),
                (sl, dl, 0, -1, pairs),
                (cu, du, 1, 0, lines),
                (cd, dd, -1, 0, lines),
            )
        ):
            copy = pltpu.make_async_remote_copy(
                src_ref=src.at[part],
                dst_ref=dst.at[part],
                send_sem=sems[0].at[4 * g + k],
                recv_sem=sems[1].at[4 * g + k],
                device_id=(c_of[dc], s_of[ds]),
                device_id_type=MESH,
            )
            out.append((dc, copy))
        return out

    u_copies = [
        exchange(((usr, usl, ucu, ucd), (vsr, vsl, vcu, vcd)), (u_send, u_recv), g)
        for g in range(3)
    ]
    f_copies = [
        exchange(((fsr, fsl, fcu, fcd), (hsr, hsl, hcu, hcd)), (f_send, f_recv), g)
        for g in range(3)
    ]

    def start(copies):
        for dc, copy in copies:
            guarded(exists(dc), copy.start)

    def arrive(copies):
        for dc, copy in copies:
            guarded(exists(-dc), copy.wait_recv)

    def sent(copies):
        for dc, copy in copies:
            guarded(exists(dc), copy.wait_send)

    for g in range(3):
        start(u_copies[g])

    for dc, ds, copy in eps_copies:
        guarded(exists(-dc), copy.wait_recv)

    around = {(0, 0): eps[...]}
    for k, (dc, ds) in enumerate(SPOTS):
        value = eps_in[k]
        cond = exists(-dc)
        if cond is not None:
            value = jnp.where(cond, value, jnp.zeros_like(value))
        around[(-dc, -ds)] = value
    faces = {}
    for dc in (-1, 0, 1):
        mid, left, right = around[(dc, 0)], around[(dc, -1)], around[(dc, 1)]
        before = jnp.where(low_j, rows_roll(left, -1), rows_roll(mid, 1))
        after = jnp.where(low_j, rows_roll(mid, -1), rows_roll(right, 1))
        beyond = jnp.where(low_j, left, right)
        faces[dc] = (
            jnp.maximum(before, mid),
            jnp.maximum(mid, after),
            jnp.maximum(beyond, jnp.where(low_j, before, after)),
        )

    def normal_pair(x):
        zero = jnp.zeros_like(x)
        return (
            jnp.maximum(x, jnp.where(first_lane, zero, lanes_roll(x, 1))),
            jnp.maximum(x, jnp.where(last_lane, zero, lanes_roll(x, -1))),
        )

    corner = {}
    span_far = {}
    chord_far = {}
    for k in range(3):
        below, mid, above = faces[-1][k], faces[0][k], faces[1][k]
        before = jnp.where(row_lo, rows_roll(below, 2), rows_roll(mid, 2))
        after = jnp.where(row_hi, rows_roll(above, -2), rows_roll(mid, -2))
        for sx, value in ((0, jnp.maximum(before, mid)), (1, jnp.maximum(mid, after))):
            pair = normal_pair(value)
            for sz in range(2):
                if k == 2:
                    span_far[(sx, sz)] = pair[sz]
                else:
                    corner[(sx, k, sz)] = pair[sz]
        if k < 2:
            beyond = jnp.where(row_lo, rows_roll(below, 4), rows_roll(above, 4))
            pair = normal_pair(jnp.maximum(beyond, jnp.where(row_lo, before, after)))
            for sz in range(2):
                chord_far[(k, sz)] = pair[sz]

    def between(lo, hi):
        step = hi - lo
        return [lo + float(UPPER[i]) * step for i in range(5)]

    plane = {
        (sy, sz): between(corner[(0, sy, sz)], corner[(1, sy, sz)])
        for sy in range(2)
        for sz in range(2)
    }
    for a in range(5):
        edge = [between(plane[(0, sz)][a], plane[(1, sz)][a]) for sz in range(2)]
        for b in range(5):
            vis[pl.ds(25 * a + 5 * b, 5)] = jnp.stack(between(edge[0][b], edge[1][b]))
    weight = {}
    for sx in range(2):
        for sz in range(2):
            near = jnp.where(low_j, corner[(sx, 0, sz)], corner[(sx, 1, sz)])
            value = K_FAR * span_far[(sx, sz)] + K_NEAR * near
            weight[(sx, sz)] = jnp.where(low_j, value, -value)
    edge = [between(weight[(0, sz)], weight[(1, sz)]) for sz in range(2)]
    for a in range(5):
        ks[pl.ds(5 * a, 5)] = jnp.stack(between(edge[0][a], edge[1][a]))
    for sy in range(2):
        for sz in range(2):
            near = jnp.where(row_lo, corner[(0, sy, sz)], corner[(1, sy, sz)])
            value = K_FAR * chord_far[(sy, sz)] + K_NEAR * near
            weight[(sy, sz)] = jnp.where(row_lo, value, -value)
    edge = [between(weight[(0, sz)], weight[(1, sz)]) for sz in range(2)]
    for b in range(5):
        kc[pl.ds(5 * b, 5)] = jnp.stack(between(edge[0][b], edge[1][b]))

    span_trace = [jnp.where(low_j, float(LEFT[b]), float(RIGHT[b])) for b in range(5)]
    chord_trace = [jnp.where(row_lo, float(LEFT[a]), float(RIGHT[a])) for a in range(5)]
    span_lift = [jnp.where(low_j, float(HALF_L[b]), float(HALF_R[b])) for b in range(5)]
    chord_lift = [
        jnp.where(row_lo, float(HALF_L[a]), jnp.where(row_hi, float(HALF_R[a]), 0.0))
        for a in range(5)
    ]

    def flux_traces(k, carry):
        v = k // 5
        a = k - 5 * v
        at = [pl.ds(25 * a + 5 * b, 5) for b in range(5)]
        acc = None
        for b in range(5):
            term = span_trace[b][None] * (vis[at[b]] * gs[v, at[b]])
            acc = term if acc is None else acc + term
        tsf[pl.ds(25 * v + 5 * a, 5)] = acc
        at = [pl.ds(25 * i + 5 * a, 5) for i in range(5)]
        acc = None
        for i in range(5):
            term = chord_trace[i][None] * (vis[at[i]] * gc[v, at[i]])
            acc = term if acc is None else acc + term
        q = 25 * v + 5 * a
        fcu[pl.ds(q, 5)] = acc[:, 6:8]
        fcd[pl.ds(q, 5)] = acc[:, 0:2]
        return carry

    for g, (v0, v1) in enumerate(GROUPS):
        lax.fori_loop(5 * v0, 5 * v1, flux_traces, 0)
        pack(tsf, fsr, fsl, 25 * v0 // 2, -(-25 * (v1 - v0) // 2))
        start(f_copies[g])

    def normal_part(k, carry):
        v = k // 5
        a = k - 5 * v
        block = gn[v, pl.ds(25 * a, 25)] * vis[pl.ds(25 * a, 25)]
        block = block.reshape(5, 5, 8, 128)
        eo = even_odd([block[:, i] for i in range(5)])
        tl, tr = line_traces(eo)
        out = line_apply(
            eo,
            pick(first_lane, -tl, lanes_roll(tr, 1)),
            pick(last_lane, -tr, lanes_roll(tl, -1)),
        )
        for b in range(5):
            r[v, pl.ds(25 * a + 5 * b, 5)] = jnp.stack([out[i][b] for i in range(5)])
        return carry

    lax.fori_loop(0, 25, normal_part, 0)

    end_lo = jnp.logical_and(row_lo, jnp.logical_not(has_lo))
    end_hi = jnp.logical_and(row_hi, jnp.logical_not(has_hi))

    def unpack_all(from_left, from_right, dst, start_pair, count):
        def body(k, carry):
            p = start_pair + k
            first, second = unpack(from_left, from_right, p)
            dst[2 * p] = first
            dst[2 * p + 1] = second
            return carry

        lax.fori_loop(0, count, body, 0)

    def chord_outer(from_lo, from_hi, q):
        lo = from_lo[pl.ds(q, 5)]
        hi = from_hi[pl.ds(q, 5)]
        gap = jnp.zeros((5, 4, 128), jnp.float32)
        return jnp.concatenate([lo, gap, hi], axis=1)

    def span_part(k, carry):
        v = k // 5
        a = k - 5 * v
        outer = tsf[pl.ds(25 * v + 5 * a, 5)]
        flux = [
            vis[pl.ds(25 * a + 5 * b, 5)]
            * (gs[v, pl.ds(25 * a + 5 * b, 5)] + span_lift[b][None] * outer)
            for b in range(5)
        ]
        eo = even_odd(flux)
        tl, tr = line_traces(eo)
        zero = jnp.zeros_like(tl)
        out = line_apply(
            eo, pick(low_j, zero, rows_roll(tr, 1)), pick(low_j, rows_roll(tl, -1), zero)
        )
        for b in range(5):
            at = pl.ds(25 * a + 5 * b, 5)
            r[v, at] = r[v, at] + out[b]
        return carry

    def chord_part(k, carry):
        v = k // 5
        b = k - 5 * v
        q = 25 * v + 5 * b
        own = tc[pl.ds(q, 5)]
        outer = chord_outer(vcu, vcd, q)
        outer = pick(jnp.logical_or(end_lo, end_hi), own, outer)
        flux = [
            vis[pl.ds(25 * a + 5 * b, 5)]
            * (gc[v, pl.ds(25 * a + 5 * b, 5)] + chord_lift[a][None] * outer)
            for a in range(5)
        ]
        eo = even_odd(flux)
        tl, tr = line_traces(eo)
        zero = jnp.zeros_like(tl)
        out = line_apply(
            eo,
            pick(row_lo, pick(end_lo, -tl, zero), rows_roll(tr, 2)),
            pick(row_hi, pick(end_hi, -tr, zero), rows_roll(tl, -2)),
        )
        for a in range(5):
            at = pl.ds(25 * a + 5 * b, 5)
            r[v, at] = r[v, at] + out[a]
        return carry

    for g, (v0, v1) in enumerate(GROUPS):
        arrive(u_copies[g])
        unpack_all(vsr, vsl, tsf, 25 * v0 // 2, -(-25 * (v1 - v0) // 2))
        lax.fori_loop(5 * v0, 5 * v1, span_part, 0)
        lax.fori_loop(5 * v0, 5 * v1, chord_part, 0)

    def finish(k, carry):
        v = k // 5
        a = k - 5 * v
        q = 25 * v + 5 * a
        outer = tsf[pl.ds(q, 5)] + ks[pl.ds(5 * a, 5)] * ts[pl.ds(q, 5)]
        for b in range(5):
            at = pl.ds(25 * a + 5 * b, 5)
            r[v, at] = r[v, at] + span_lift[b][None] * outer
        return carry

    def finish_chord(k, carry):
        v = k // 5
        b = k - 5 * v
        q = 25 * v + 5 * b
        outer = chord_outer(hcu, hcd, q) + kc[pl.ds(5 * b, 5)] * tc[pl.ds(q, 5)]
        outer = pick(jnp.logical_or(end_lo, end_hi), jnp.zeros_like(outer), outer)
        for a in range(5):
            at = pl.ds(25 * a + 5 * b, 5)
            r[v, at] = r[v, at] + chord_lift[a][None] * outer
        return carry

    for g, (v0, v1) in enumerate(GROUPS):
        arrive(f_copies[g])
        unpack_all(hsr, hsl, tsf, 25 * v0 // 2, -(-25 * (v1 - v0) // 2))
        lax.fori_loop(5 * v0, 5 * v1, finish, 0)
        lax.fori_loop(5 * v0, 5 * v1, finish_chord, 0)
    for dc, ds, copy in eps_copies:
        guarded(exists(dc), copy.wait_send)
    for g in range(3):
        sent(u_copies[g])
        sent(f_copies[g])


def store_kernel(r, vis, res_hbm, vis_hbm, sem):
    copies = [
        pltpu.make_async_copy(r.at[v], res_hbm.at[v], sem.at[v]) for v in range(5)
    ] + [pltpu.make_async_copy(vis, vis_hbm, sem.at[5])]
    for copy in copies:
        copy.start()
    for copy in copies:
        copy.wait()


def shards(state):
    chords, spans = lax.axis_size("chord"), lax.axis_size("span")
    f32 = jnp.float32
    field = pltpu.VMEM((5, 125, 8, 128), f32)
    pairs = pltpu.VMEM((PAIRS, 8, 128), f32)
    thin = pltpu.VMEM((132, 2, 128), f32)
    sem = pltpu.SemaphoreType.DMA
    partial, viscosity = pl.pallas_call(
        functools.partial(kernel, chords, spans),
        out_shape=(
            jax.ShapeDtypeStruct((5, 125, 8, 128), f32),
            jax.ShapeDtypeStruct((125, 8, 128), f32),
        ),
        in_specs=[pl.BlockSpec(memory_space=pltpu.HBM)],
        out_specs=(pl.BlockSpec(memory_space=pltpu.VMEM), pl.BlockSpec(memory_space=pltpu.VMEM)),
        scratch_shapes=[
            field,
            field,
            field,
            field,
            pltpu.VMEM((125, 8, 128), f32),
            pltpu.VMEM((126, 8, 128), f32),
            pltpu.VMEM((125, 8, 128), f32),
            pltpu.VMEM((126, 8, 128), f32),
        ]
        + [pairs, pairs, thin, thin] * 4
        + [
            pltpu.VMEM((8, 128), f32),
            pltpu.VMEM((8, 8, 128), f32),
            pltpu.VMEM((25, 8, 128), f32),
            pltpu.VMEM((25, 8, 128), f32),
            sem((5,)),
            sem((8,)),
            sem((8,)),
            sem((12,)),
            sem((12,)),
            sem((12,)),
            sem((12,)),
        ],
        compiler_params=pltpu.CompilerParams(
            collective_id=0, has_side_effects=True, vmem_limit_bytes=40 * 1024 * 1024
        ),
        name="viscous",
    )(pltpu.with_memory_space_constraint(state.reshape(5, 125, 8, 128), pltpu.HBM))
    residual, viscosity = pl.pallas_call(
        store_kernel,
        out_shape=(
            jax.ShapeDtypeStruct((5, 125, 8, 128), f32),
            jax.ShapeDtypeStruct((125, 8, 128), f32),
        ),
        in_specs=[pl.BlockSpec(memory_space=pltpu.VMEM)] * 2,
        out_specs=(pl.BlockSpec(memory_space=pl.ANY), pl.BlockSpec(memory_space=pl.ANY)),
        scratch_shapes=[sem((6,))],
        compiler_params=pltpu.CompilerParams(vmem_limit_bytes=4 * 1024 * 1024),
        name="store",
    )(partial, viscosity)
    return residual.reshape(state.shape), viscosity.reshape(state.shape[1:])


def solution(mesh):
    in_specs = (P(None, None, "chord", "span", None),)
    out_specs = (P(None, None, "chord", "span", None), P(None, "chord", "span", None))
    return jax.shard_map(shards, mesh=mesh, in_specs=in_specs, out_specs=out_specs, check_vma=False)
```

```python
import functools
import math

import jax
import jax.numpy as jnp
import numpy as np
from jax import lax
from jax.experimental import pallas as pl
from jax.experimental.pallas import tpu as pltpu
from jax.sharding import PartitionSpec as P

MESH = pl.DeviceIdType.MESH
EPS_SCALE = 0.01
SENSOR_CENTRE = -3.0
SENSOR_WIDTH = 1.5
RATIO_FLOOR = 1e-06
ENERGY_EPS = 1e-06
NODES = [-0.906179845938664, -0.5384693101056831, 0.0, 0.5384693101056831, 0.906179845938664]
WEIGHTS = [
    0.2369268850561891,
    0.4786286704993665,
    0.5688888888888889,
    0.4786286704993665,
    0.2369268850561891,
]


def legendre_values(points):
    values = [np.ones(points.shape), np.array(points)]
    for order in range(1, 5):
        values.append(
            ((2 * order + 1) * points * values[order] - order * values[order - 1]) / (order + 1)
        )
    return values


def tables():
    x = np.array(NODES)
    w = np.array(WEIGHTS)
    bary = np.array([1.0 / np.prod([x[j] - x[k] for k in range(5) if k != j]) for j in range(5)])
    deriv = np.zeros((5, 5))
    for i in range(5):
        for j in range(5):
            if i != j:
                deriv[i, j] = bary[j] / bary[i] / (x[i] - x[j])
        deriv[i, i] = -np.sum(deriv[i])
    left = np.ones(5)
    right = np.ones(5)
    for j in range(5):
        for k in range(5):
            if k != j:
                left[j] *= (-1.0 - x[k]) / (x[j] - x[k])
                right[j] *= (1.0 - x[k]) / (x[j] - x[k])
    legendre = legendre_values(x)
    fourth = 7.0 * legendre[3] + 3.0 * legendre[1]
    fifth = 9.0 * legendre[4] + 5.0 * legendre[2] + legendre[0]
    half_l = 0.25 * (fourth - fifth)
    half_r = 0.25 * (fourth + fifth)
    modal = np.zeros((5, 5))
    for k in range(5):
        modal[k, :] = w * math.sqrt((2 * k + 1) / 2.0) * legendre[k]
    own = deriv - np.outer(half_l, left) - np.outer(half_r, right)
    upper = (1.0 + x) / 2.0
    near = float(np.sum(right * half_r * upper))
    far = float(np.sum(right * half_r * (1.0 - upper)))
    return own, left, right, half_l, half_r, modal, upper, near, far


OWN, LEFT, RIGHT, HALF_L, HALF_R, MODAL, UPPER, K_NEAR, K_FAR = tables()


def even_odd(u):
    return u[0] + u[4], u[1] + u[3], u[0] - u[4], u[1] - u[3], u[2]


def line_traces(eo):
    s0, s1, d0, d1, m = eo
    even = (
        float((RIGHT[0] + RIGHT[4]) / 2) * s0
        + float((RIGHT[1] + RIGHT[3]) / 2) * s1
        + float(RIGHT[2]) * m
    )
    odd = float((RIGHT[0] - RIGHT[4]) / 2) * d0 + float((RIGHT[1] - RIGHT[3]) / 2) * d1
    return even - odd, even + odd


def line_apply(eo, prev, following):
    s0, s1, d0, d1, m = eo
    sp = prev + following
    dp = prev - following
    out = [None] * 5
    for i in (0, 1):
        a = [(OWN[i, j] + OWN[i, 4 - j]) / 2 for j in (0, 1)]
        b = [(OWN[i, j] - OWN[i, 4 - j]) / 2 for j in (0, 1)]
        p = (
            float(a[0]) * s0
            + float(a[1]) * s1
            + float(OWN[i, 2]) * m
            + float((HALF_L[i] + HALF_R[i]) / 2) * sp
        )
        q = float(b[0]) * d0 + float(b[1]) * d1 + float((HALF_L[i] - HALF_R[i]) / 2) * dp
        out[i] = p + q
        out[4 - i] = q - p
    b = [(OWN[2, j] - OWN[2, 4 - j]) / 2 for j in (0, 1)]
    out[2] = float(b[0]) * d0 + float(b[1]) * d1 + float((HALF_L[2] - HALF_R[2]) / 2) * dp
    return out


def modal_line(u):
    s0, s1, d0, d1, m = even_odd(u)
    out = []
    for k in range(5):
        if k % 2 == 0:
            out.append(
                float(MODAL[k, 0]) * s0 + float(MODAL[k, 1]) * s1 + float(MODAL[k, 2]) * m
            )
        else:
            out.append(float(MODAL[k, 0]) * d0 + float(MODAL[k, 1]) * d1)
    return out


def rows_roll(x, shift):
    return pltpu.roll(x, shift % 8, axis=x.ndim - 2)


def lanes_roll(x, shift):
    return pltpu.roll(x, shift % 128, axis=x.ndim - 1)


GROUPS = ((0, 2), (2, 4), (4, 5))
PAIRS = 63
ROUTES = {("u", 0): 0, ("u", 1): 1, ("u", 2): 2}
RELAYS = tuple(ROUTES)
SPOTS = tuple((dc, ds) for dc in (-1, 0, 1) for ds in (-1, 0, 1) if (dc, ds) != (0, 0))


def kernel(
    chords,
    spans,
    x_hbm,
    r,
    vis,
    u,
    gs,
    gc,
    gn,
    modes,
    ts,
    tc,
    tsf,
    usr,
    usl,
    ucu,
    ucd,
    vsr,
    vsl,
    vcu,
    vcd,
    fsr,
    fsl,
    fcu,
    fcd,
    hsr,
    hsl,
    hcu,
    hcd,
    held,
    eps,
    eps_in,
    ks,
    kc,
    load_sem,
    e_send,
    e_recv,
    u_send,
    u_recv,
    f_send,
    f_recv,
    h_send,
    h_recv,
):
    c = lax.axis_index("chord")
    s = lax.axis_index("span")
    has_lo = c > 0
    has_hi = c < chords - 1
    s_of = {0: s, 1: lax.rem(s + 1, spans), -1: lax.rem(s + spans - 1, spans)}
    c_of = {0: c, 1: lax.rem(c + 1, chords), -1: lax.rem(c + chords - 1, chords)}

    def exists(dc):
        return {0: None, 1: has_hi, -1: has_lo}[dc]

    def guarded(cond, action):
        if cond is None:
            action()
        else:
            pl.when(cond)(action)

    barrier = pltpu.get_barrier_semaphore()
    for dc, ds in SPOTS:
        guarded(
            exists(dc),
            lambda dc=dc, ds=ds: pl.semaphore_signal(
                barrier, inc=1, device_id=(c_of[dc], s_of[ds]), device_id_type=MESH
            ),
        )

    half = chords // 2
    is_up = c == half - 1
    is_down = c == half
    stations = sorted(set(ROUTES.values()))

    def meet(cond, others):
        for other in others:
            pl.when(cond)(
                lambda other=other: pl.semaphore_signal(
                    barrier, inc=1, device_id=(other, s), device_id_type=MESH
                )
            )
        return jnp.where(cond, len(others), 0)

    last = chords - 1
    extra = 0
    for at, others in (
        (half - 1, [t for t in stations if t != half - 2] + [last - t for t in stations]),
        (half, [last - t for t in stations if t != half - 2] + [t for t in stations]),
    ):
        extra = extra + meet(c == at, others)
    for t in stations:
        near = [] if t == half - 2 else [half - 1]
        extra = extra + meet(c == t, near + [half])
        near = [] if t == half - 2 else [half]
        extra = extra + meet(c == last - t, near + [half - 1])

    loads = [pltpu.make_async_copy(x_hbm.at[v], u.at[v], load_sem.at[v]) for v in range(5)]
    for copy in loads:
        copy.start()

    row = lax.broadcasted_iota(jnp.int32, (8, 128), 0)
    lane = lax.broadcasted_iota(jnp.int32, (8, 128), 1)
    low_j = lax.rem(row, 2) == 0
    row_lo = row < 2
    row_hi = row >= 6
    first_lane = lane == 0
    last_lane = lane == 127

    def pick(mask, a, b):
        if a.ndim == 3:
            mask = jnp.broadcast_to(mask[None], a.shape)
        return jnp.where(mask, a, b)

    loads[0].wait()

    def modes_cb(a, carry):
        block = u[0, pl.ds(25 * a, 25)].reshape(5, 5, 8, 128)
        along_c = modal_line([block[:, k] for k in range(5)])
        stacked = [jnp.stack([along_c[o][b] for o in range(5)]) for b in range(5)]
        along_b = modal_line(stacked)
        for n in range(5):
            modes[pl.ds(25 * a + 5 * n, 5)] = along_b[n]
        return carry

    lax.fori_loop(0, 5, modes_cb, 0)
    low = jnp.zeros((4, 8, 128), jnp.float32)
    high = jnp.zeros((8, 128), jnp.float32)
    high4 = jnp.zeros((5, 8, 128), jnp.float32)
    for n in range(5):
        along_a = modal_line([modes[25 * a + 5 * n : 25 * a + 5 * n + 5] for a in range(5)])
        for m in range(5):
            square = along_a[m] * along_a[m]
            if n == 4 or m == 4:
                high4 = high4 + square
            else:
                low = low + square[:4]
                high = high + square[4]
    high = high + (high4[0] + high4[1]) + (high4[2] + high4[3]) + high4[4]
    total = (low[0] + low[1]) + (low[2] + low[3]) + high
    ratio = high / (total + ENERGY_EPS)
    level = jnp.log(jnp.maximum(ratio, RATIO_FLOOR)) * (1.0 / math.log(10.0))
    ramp = jnp.clip((level - SENSOR_CENTRE) / SENSOR_WIDTH, -1.0, 1.0)
    eps[...] = (EPS_SCALE * 0.5) * (1.0 + jnp.sin((0.5 * math.pi) * ramp))

    for v in range(1, 5):
        loads[v].wait()

    span_trace = [jnp.where(low_j, float(LEFT[b]), float(RIGHT[b])) for b in range(5)]
    chord_trace = [jnp.where(row_lo, float(LEFT[a]), float(RIGHT[a])) for a in range(5)]
    span_lift = [jnp.where(low_j, float(HALF_L[b]), float(HALF_R[b])) for b in range(5)]
    chord_lift = [
        jnp.where(row_lo, float(HALF_L[a]), jnp.where(row_hi, float(HALF_R[a]), 0.0))
        for a in range(5)
    ]

    def outer_traces(k, carry):
        v = k // 5
        i = k - 5 * v
        q = 25 * v + 5 * i
        acc = None
        for b in range(5):
            term = span_trace[b][None] * u[v, pl.ds(25 * i + 5 * b, 5)]
            acc = term if acc is None else acc + term
        ts[pl.ds(q, 5)] = acc
        acc = None
        for a in range(5):
            term = chord_trace[a][None] * u[v, pl.ds(25 * a + 5 * i, 5)]
            acc = term if acc is None else acc + term
        tc[pl.ds(q, 5)] = acc
        ucu[pl.ds(q, 5)] = acc[:, 6:8]
        ucd[pl.ds(q, 5)] = acc[:, 0:2]
        return carry

    lax.fori_loop(0, 25, outer_traces, 0)
    ts[125] = jnp.zeros((8, 128), jnp.float32)
    tsf[125] = jnp.zeros((8, 128), jnp.float32)

    def pack(src, to_right, to_left, first, count, step):
        def body(k, carry):
            p = first + step * k
            two = src[pl.ds(2 * p, 2 * step)].reshape(step, 2, 8, 128)
            one, other = two[:, 0], two[:, 1]
            to_right[pl.ds(p, step)] = pick(low_j, rows_roll(one, -1), other)
            to_left[pl.ds(p, step)] = pick(low_j, one, rows_roll(other, 1))
            return carry

        lax.fori_loop(0, count // step, body, 0)

    pack(ts, usr, usl, 0, PAIRS, 9)

    pl.semaphore_wait(barrier, 2 + jnp.where(has_lo, 3, 0) + jnp.where(has_hi, 3, 0) + extra)

    eps_copies = []
    for k, (dc, ds) in enumerate(SPOTS):
        copy = pltpu.make_async_remote_copy(
            src_ref=eps,
            dst_ref=eps_in.at[k],
            send_sem=e_send.at[k],
            recv_sem=e_recv.at[k],
            device_id=(c_of[dc], s_of[ds]),
            device_id_type=MESH,
        )
        guarded(exists(dc), copy.start)
        eps_copies.append((dc, ds, copy))

    def exchange(kind, g):
        (sr, sl, cu, cd), (dr, dl, du, dd), sems = messages[kind]
        v0, v1 = GROUPS[g]
        pairs = pl.ds(25 * v0 // 2, -(-25 * (v1 - v0) // 2))
        lines = pl.ds(25 * v0, 25 * (v1 - v0))
        out = []
        for k, (src, dst, dc, ds, part) in enumerate(
            (
                (sr, dr, 0, 1, pairs),
                (sl, dl, 0, -1, pairs),
                (cu, du, 1, 0, lines),
                (cd, dd, -1, 0, lines),
            )
        ):
            copy = pltpu.make_async_remote_copy(
                src_ref=src.at[part],
                dst_ref=dst.at[part],
                send_sem=sems[0].at[4 * g + k],
                recv_sem=sems[1].at[4 * g + k],
                device_id=(c_of[dc], s_of[ds]),
                device_id_type=MESH,
            )
            first = None
            if dc != 0 and (kind, g) in ROUTES:
                t = ROUTES[(kind, g)]
                n = RELAYS.index((kind, g))
                crossing = is_up if dc == 1 else is_down
                first = pltpu.make_async_remote_copy(
                    src_ref=src.at[part],
                    dst_ref=held.at[part],
                    send_sem=sems[0].at[4 * g + k],
                    recv_sem=h_recv.at[n],
                    device_id=(t if dc == 1 else last - t, s),
                    device_id_type=MESH,
                )
                second = pltpu.make_async_remote_copy(
                    src_ref=held.at[part],
                    dst_ref=dst.at[part],
                    send_sem=h_send.at[n],
                    recv_sem=sems[1].at[4 * g + k],
                    device_id=(half if dc == 1 else half - 1, s),
                    device_id_type=MESH,
                )
                first = (crossing, c == (t if dc == 1 else last - t), first, second)
            out.append((dc, copy, first))
        return out

    messages = {
        "u": ((usr, usl, ucu, ucd), (vsr, vsl, vcu, vcd), (u_send, u_recv)),
        "f": ((fsr, fsl, fcu, fcd), (hsr, hsl, hcu, hcd), (f_send, f_recv)),
    }
    u_copies = [exchange("u", g) for g in range(3)]
    f_copies = [exchange("f", g) for g in range(3)]

    def start(copies):
        for dc, copy, relay in copies:
            cond = exists(dc)
            if relay is not None:
                pl.when(relay[0])(relay[2].start)
                cond = jnp.logical_and(cond, jnp.logical_not(relay[0]))
            guarded(cond, copy.start)

    def pass_on(copies):
        for dc, copy, relay in copies:
            if relay is not None:

                def forward(relay=relay):
                    relay[2].wait_recv()
                    relay[3].start()

                pl.when(relay[1])(forward)

    def arrive(copies):
        for dc, copy, relay in copies:
            guarded(exists(-dc), copy.wait_recv)

    def sent(copies):
        for dc, copy, relay in copies:
            guarded(exists(dc), copy.wait_send)
            if relay is not None:
                pl.when(relay[1])(relay[3].wait_send)

    for g in range(3):
        start(u_copies[g])

    def local_ab(k, carry):
        v = k // 5
        a = k - 5 * v
        block = u[v, pl.ds(25 * a, 25)].reshape(5, 5, 8, 128)
        eo = even_odd([block[b] for b in range(5)])
        tl, tr = line_traces(eo)
        zero = jnp.zeros_like(tl)
        grad = line_apply(
            eo, pick(low_j, zero, rows_roll(tr, 1)), pick(low_j, rows_roll(tl, -1), zero)
        )
        for b in range(5):
            gs[v, pl.ds(25 * a + 5 * b, 5)] = grad[b]
        eo = even_odd([block[:, k] for k in range(5)])
        tl, tr = line_traces(eo)
        grad = line_apply(
            eo,
            pick(first_lane, tl, lanes_roll(tr, 1)),
            pick(last_lane, tr, lanes_roll(tl, -1)),
        )
        for b in range(5):
            gn[v, pl.ds(25 * a + 5 * b, 5)] = jnp.stack([grad[k][b] for k in range(5)])
        return carry

    lax.fori_loop(0, 25, local_ab, 0)

    def local_c(k, carry):
        v = k // 5
        b = k - 5 * v
        eo = even_odd([u[v, pl.ds(25 * a + 5 * b, 5)] for a in range(5)])
        tl, tr = line_traces(eo)
        zero = jnp.zeros_like(tl)
        grad = line_apply(
            eo, pick(row_lo, zero, rows_roll(tr, 2)), pick(row_hi, zero, rows_roll(tl, -2))
        )
        for a in range(5):
            gc[v, pl.ds(25 * a + 5 * b, 5)] = grad[a]
        return carry

    lax.fori_loop(0, 25, local_c, 0)
    for g in range(3):
        pass_on(u_copies[g])

    for dc, ds, copy in eps_copies:
        guarded(exists(-dc), copy.wait_recv)

    around = {(0, 0): eps[...]}
    for k, (dc, ds) in enumerate(SPOTS):
        value = eps_in[k]
        cond = exists(-dc)
        if cond is not None:
            value = jnp.where(cond, value, jnp.zeros_like(value))
        around[(-dc, -ds)] = value
    faces = {}
    for dc in (-1, 0, 1):
        mid, left, right = around[(dc, 0)], around[(dc, -1)], around[(dc, 1)]
        before = jnp.where(low_j, rows_roll(left, -1), rows_roll(mid, 1))
        after = jnp.where(low_j, rows_roll(mid, -1), rows_roll(right, 1))
        beyond = jnp.where(low_j, left, right)
        faces[dc] = (
            jnp.maximum(before, mid),
            jnp.maximum(mid, after),
            jnp.maximum(beyond, jnp.where(low_j, before, after)),
        )

    def normal_pair(x):
        zero = jnp.zeros_like(x)
        return (
            jnp.maximum(x, jnp.where(first_lane, zero, lanes_roll(x, 1))),
            jnp.maximum(x, jnp.where(last_lane, zero, lanes_roll(x, -1))),
        )

    corner = {}
    span_far = {}
    chord_far = {}
    for k in range(3):
        below, mid, above = faces[-1][k], faces[0][k], faces[1][k]
        before = jnp.where(row_lo, rows_roll(below, 2), rows_roll(mid, 2))
        after = jnp.where(row_hi, rows_roll(above, -2), rows_roll(mid, -2))
        for sx, value in ((0, jnp.maximum(before, mid)), (1, jnp.maximum(mid, after))):
            pair = normal_pair(value)
            for sz in range(2):
                if k == 2:
                    span_far[(sx, sz)] = pair[sz]
                else:
                    corner[(sx, k, sz)] = pair[sz]
        if k < 2:
            beyond = jnp.where(row_lo, rows_roll(below, 4), rows_roll(above, 4))
            pair = normal_pair(jnp.maximum(beyond, jnp.where(row_lo, before, after)))
            for sz in range(2):
                chord_far[(k, sz)] = pair[sz]

    def between(lo, hi):
        step = hi - lo
        return [lo + float(UPPER[i]) * step for i in range(5)]

    plane = {
        (sy, sz): between(corner[(0, sy, sz)], corner[(1, sy, sz)])
        for sy in range(2)
        for sz in range(2)
    }
    for a in range(5):
        edge = [between(plane[(0, sz)][a], plane[(1, sz)][a]) for sz in range(2)]
        for b in range(5):
            vis[pl.ds(25 * a + 5 * b, 5)] = jnp.stack(between(edge[0][b], edge[1][b]))
    weight = {}
    for sx in range(2):
        for sz in range(2):
            near = jnp.where(low_j, corner[(sx, 0, sz)], corner[(sx, 1, sz)])
            value = K_FAR * span_far[(sx, sz)] + K_NEAR * near
            weight[(sx, sz)] = jnp.where(low_j, value, -value)
    edge = [between(weight[(0, sz)], weight[(1, sz)]) for sz in range(2)]
    for a in range(5):
        ks[pl.ds(5 * a, 5)] = jnp.stack(between(edge[0][a], edge[1][a]))
    for sy in range(2):
        for sz in range(2):
            near = jnp.where(row_lo, corner[(0, sy, sz)], corner[(1, sy, sz)])
            value = K_FAR * chord_far[(sy, sz)] + K_NEAR * near
            weight[(sy, sz)] = jnp.where(row_lo, value, -value)
    edge = [between(weight[(0, sz)], weight[(1, sz)]) for sz in range(2)]
    for b in range(5):
        kc[pl.ds(5 * b, 5)] = jnp.stack(between(edge[0][b], edge[1][b]))

    def flux_traces(k, carry):
        v = k // 5
        a = k - 5 * v
        at = [pl.ds(25 * a + 5 * b, 5) for b in range(5)]
        acc = None
        for b in range(5):
            term = span_trace[b][None] * (vis[at[b]] * gs[v, at[b]])
            acc = term if acc is None else acc + term
        tsf[pl.ds(25 * v + 5 * a, 5)] = acc
        at = [pl.ds(25 * i + 5 * a, 5) for i in range(5)]
        acc = None
        for i in range(5):
            term = chord_trace[i][None] * (vis[at[i]] * gc[v, at[i]])
            acc = term if acc is None else acc + term
        q = 25 * v + 5 * a
        fcu[pl.ds(q, 5)] = acc[:, 6:8]
        fcd[pl.ds(q, 5)] = acc[:, 0:2]
        return carry

    for g, (v0, v1) in enumerate(GROUPS):
        lax.fori_loop(5 * v0, 5 * v1, flux_traces, 0)
        count = -(-25 * (v1 - v0) // 2)
        pack(tsf, fsr, fsl, 25 * v0 // 2, count, 5 if count % 5 == 0 else count)
        start(f_copies[g])

    def normal_part(k, carry):
        v = k // 5
        a = k - 5 * v
        block = gn[v, pl.ds(25 * a, 25)] * vis[pl.ds(25 * a, 25)]
        block = block.reshape(5, 5, 8, 128)
        eo = even_odd([block[:, i] for i in range(5)])
        tl, tr = line_traces(eo)
        out = line_apply(
            eo,
            pick(first_lane, -tl, lanes_roll(tr, 1)),
            pick(last_lane, -tr, lanes_roll(tl, -1)),
        )
        for b in range(5):
            r[v, pl.ds(25 * a + 5 * b, 5)] = jnp.stack([out[i][b] for i in range(5)])
        return carry

    lax.fori_loop(0, 25, normal_part, 0)

    end_lo = jnp.logical_and(row_lo, jnp.logical_not(has_lo))
    end_hi = jnp.logical_and(row_hi, jnp.logical_not(has_hi))

    def unpack(from_left, from_right, dst, first, count, step):
        def body(k, carry):
            p = first + step * k
            a, b = from_left[pl.ds(p, step)], from_right[pl.ds(p, step)]
            one = pick(low_j, a, rows_roll(b, 1))
            other = pick(low_j, rows_roll(a, -1), b)
            dst[pl.ds(2 * p, 2 * step)] = jnp.stack([one, other], axis=1).reshape(
                2 * step, 8, 128
            )
            return carry

        lax.fori_loop(0, count // step, body, 0)

    def chord_outer(from_lo, from_hi, q):
        lo = from_lo[pl.ds(q, 5)]
        hi = from_hi[pl.ds(q, 5)]
        gap = jnp.zeros((5, 4, 128), jnp.float32)
        return jnp.concatenate([lo, gap, hi], axis=1)

    def span_part(k, carry):
        v = k // 5
        a = k - 5 * v
        outer = tsf[pl.ds(25 * v + 5 * a, 5)]
        flux = [
            vis[pl.ds(25 * a + 5 * b, 5)]
            * (gs[v, pl.ds(25 * a + 5 * b, 5)] + span_lift[b][None] * outer)
            for b in range(5)
        ]
        eo = even_odd(flux)
        tl, tr = line_traces(eo)
        zero = jnp.zeros_like(tl)
        out = line_apply(
            eo, pick(low_j, zero, rows_roll(tr, 1)), pick(low_j, rows_roll(tl, -1), zero)
        )
        for b in range(5):
            at = pl.ds(25 * a + 5 * b, 5)
            r[v, at] = r[v, at] + out[b]
        return carry

    def chord_part(k, carry):
        v = k // 5
        b = k - 5 * v
        q = 25 * v + 5 * b
        own = tc[pl.ds(q, 5)]
        outer = chord_outer(vcu, vcd, q)
        outer = pick(jnp.logical_or(end_lo, end_hi), own, outer)
        flux = [
            vis[pl.ds(25 * a + 5 * b, 5)]
            * (gc[v, pl.ds(25 * a + 5 * b, 5)] + chord_lift[a][None] * outer)
            for a in range(5)
        ]
        eo = even_odd(flux)
        tl, tr = line_traces(eo)
        zero = jnp.zeros_like(tl)
        out = line_apply(
            eo,
            pick(row_lo, pick(end_lo, -tl, zero), rows_roll(tr, 2)),
            pick(row_hi, pick(end_hi, -tr, zero), rows_roll(tl, -2)),
        )
        for a in range(5):
            at = pl.ds(25 * a + 5 * b, 5)
            r[v, at] = r[v, at] + out[a]
        return carry

    for g, (v0, v1) in enumerate(GROUPS):
        arrive(u_copies[g])
        count = -(-25 * (v1 - v0) // 2)
        unpack(vsr, vsl, tsf, 25 * v0 // 2, count, 5 if count % 5 == 0 else count)
        lax.fori_loop(5 * v0, 5 * v1, span_part, 0)
        lax.fori_loop(5 * v0, 5 * v1, chord_part, 0)
        pass_on(f_copies[g])

    def finish(k, carry):
        v = k // 5
        a = k - 5 * v
        q = 25 * v + 5 * a
        outer = tsf[pl.ds(q, 5)] + ks[pl.ds(5 * a, 5)] * ts[pl.ds(q, 5)]
        for b in range(5):
            at = pl.ds(25 * a + 5 * b, 5)
            r[v, at] = r[v, at] + span_lift[b][None] * outer
        return carry

    def finish_chord(k, carry):
        v = k // 5
        b = k - 5 * v
        q = 25 * v + 5 * b
        outer = chord_outer(hcu, hcd, q) + kc[pl.ds(5 * b, 5)] * tc[pl.ds(q, 5)]
        outer = pick(jnp.logical_or(end_lo, end_hi), jnp.zeros_like(outer), outer)
        for a in range(5):
            at = pl.ds(25 * a + 5 * b, 5)
            r[v, at] = r[v, at] + chord_lift[a][None] * outer
        return carry

    for g, (v0, v1) in enumerate(GROUPS):
        arrive(f_copies[g])
        count = -(-25 * (v1 - v0) // 2)
        unpack(hsr, hsl, tsf, 25 * v0 // 2, count, 5 if count % 5 == 0 else count)
        lax.fori_loop(5 * v0, 5 * v1, finish, 0)
        lax.fori_loop(5 * v0, 5 * v1, finish_chord, 0)
    for dc, ds, copy in eps_copies:
        guarded(exists(dc), copy.wait_send)
    for g in range(3):
        sent(u_copies[g])
        sent(f_copies[g])


def store_kernel(r, vis, res_hbm, vis_hbm, sem):
    copies = [
        pltpu.make_async_copy(r.at[v], res_hbm.at[v], sem.at[v]) for v in range(5)
    ] + [pltpu.make_async_copy(vis, vis_hbm, sem.at[5])]
    for copy in copies:
        copy.start()
    for copy in copies:
        copy.wait()


def shards(state):
    chords, spans = lax.axis_size("chord"), lax.axis_size("span")
    f32 = jnp.float32
    field = pltpu.VMEM((5, 125, 8, 128), f32)
    pairs = pltpu.VMEM((PAIRS, 8, 128), f32)
    thin = pltpu.VMEM((132, 2, 128), f32)
    sem = pltpu.SemaphoreType.DMA
    partial, viscosity = pl.pallas_call(
        functools.partial(kernel, chords, spans),
        out_shape=(
            jax.ShapeDtypeStruct((5, 125, 8, 128), f32),
            jax.ShapeDtypeStruct((125, 8, 128), f32),
        ),
        in_specs=[pl.BlockSpec(memory_space=pltpu.HBM)],
        out_specs=(pl.BlockSpec(memory_space=pltpu.VMEM), pl.BlockSpec(memory_space=pltpu.VMEM)),
        scratch_shapes=[
            field,
            field,
            field,
            field,
            pltpu.VMEM((125, 8, 128), f32),
            pltpu.VMEM((126, 8, 128), f32),
            pltpu.VMEM((125, 8, 128), f32),
            pltpu.VMEM((126, 8, 128), f32),
        ]
        + [pairs, pairs, thin, thin] * 4
        + [thin]
        + [
            pltpu.VMEM((8, 128), f32),
            pltpu.VMEM((8, 8, 128), f32),
            pltpu.VMEM((25, 8, 128), f32),
            pltpu.VMEM((25, 8, 128), f32),
            sem((5,)),
            sem((8,)),
            sem((8,)),
            sem((12,)),
            sem((12,)),
            sem((12,)),
            sem((12,)),
            sem((len(RELAYS),)),
            sem((len(RELAYS),)),
        ],
        compiler_params=pltpu.CompilerParams(
            collective_id=0, has_side_effects=True, vmem_limit_bytes=40 * 1024 * 1024
        ),
        name="viscous",
    )(pltpu.with_memory_space_constraint(state.reshape(5, 125, 8, 128), pltpu.HBM))
    residual, viscosity = pl.pallas_call(
        store_kernel,
        out_shape=(
            jax.ShapeDtypeStruct((5, 125, 8, 128), f32),
            jax.ShapeDtypeStruct((125, 8, 128), f32),
        ),
        in_specs=[pl.BlockSpec(memory_space=pltpu.VMEM)] * 2,
        out_specs=(pl.BlockSpec(memory_space=pl.ANY), pl.BlockSpec(memory_space=pl.ANY)),
        scratch_shapes=[sem((6,))],
        compiler_params=pltpu.CompilerParams(vmem_limit_bytes=4 * 1024 * 1024),
        name="store",
    )(partial, viscosity)
    return residual.reshape(state.shape), viscosity.reshape(state.shape[1:])


def solution(mesh):
    in_specs = (P(None, None, "chord", "span", None),)
    out_specs = (P(None, None, "chord", "span", None), P(None, "chord", "span", None))
    return jax.shard_map(shards, mesh=mesh, in_specs=in_specs, out_specs=out_specs, check_vma=False)
```

```python
import functools
import math

import jax
import jax.numpy as jnp
import numpy as np
from jax import lax
from jax.experimental import pallas as pl
from jax.experimental.pallas import tpu as pltpu
from jax.sharding import PartitionSpec as P

MESH = pl.DeviceIdType.MESH
EPS_SCALE = 0.01
SENSOR_CENTRE = -3.0
SENSOR_WIDTH = 1.5
RATIO_FLOOR = 1e-06
ENERGY_EPS = 1e-06
NODES = [-0.906179845938664, -0.5384693101056831, 0.0, 0.5384693101056831, 0.906179845938664]
WEIGHTS = [
    0.2369268850561891,
    0.4786286704993665,
    0.5688888888888889,
    0.4786286704993665,
    0.2369268850561891,
]


def legendre_values(points):
    values = [np.ones(points.shape), np.array(points)]
    for order in range(1, 5):
        values.append(
            ((2 * order + 1) * points * values[order] - order * values[order - 1]) / (order + 1)
        )
    return values


def tables():
    x = np.array(NODES)
    w = np.array(WEIGHTS)
    bary = np.array([1.0 / np.prod([x[j] - x[k] for k in range(5) if k != j]) for j in range(5)])
    deriv = np.zeros((5, 5))
    for i in range(5):
        for j in range(5):
            if i != j:
                deriv[i, j] = bary[j] / bary[i] / (x[i] - x[j])
        deriv[i, i] = -np.sum(deriv[i])
    left = np.ones(5)
    right = np.ones(5)
    for j in range(5):
        for k in range(5):
            if k != j:
                left[j] *= (-1.0 - x[k]) / (x[j] - x[k])
                right[j] *= (1.0 - x[k]) / (x[j] - x[k])
    legendre = legendre_values(x)
    fourth = 7.0 * legendre[3] + 3.0 * legendre[1]
    fifth = 9.0 * legendre[4] + 5.0 * legendre[2] + legendre[0]
    half_l = 0.25 * (fourth - fifth)
    half_r = 0.25 * (fourth + fifth)
    modal = np.zeros((5, 5))
    for k in range(5):
        modal[k, :] = w * math.sqrt((2 * k + 1) / 2.0) * legendre[k]
    own = deriv - np.outer(half_l, left) - np.outer(half_r, right)
    upper = (1.0 + x) / 2.0
    near = float(np.sum(right * half_r * upper))
    far = float(np.sum(right * half_r * (1.0 - upper)))
    return own, left, right, half_l, half_r, modal, upper, near, far


OWN, LEFT, RIGHT, HALF_L, HALF_R, MODAL, UPPER, K_NEAR, K_FAR = tables()


def even_odd(u):
    return u[0] + u[4], u[1] + u[3], u[0] - u[4], u[1] - u[3], u[2]


def line_traces(eo):
    s0, s1, d0, d1, m = eo
    even = (
        float((RIGHT[0] + RIGHT[4]) / 2) * s0
        + float((RIGHT[1] + RIGHT[3]) / 2) * s1
        + float(RIGHT[2]) * m
    )
    odd = float((RIGHT[0] - RIGHT[4]) / 2) * d0 + float((RIGHT[1] - RIGHT[3]) / 2) * d1
    return even - odd, even + odd


def line_apply(eo, prev, following):
    s0, s1, d0, d1, m = eo
    sp = prev + following
    dp = prev - following
    out = [None] * 5
    for i in (0, 1):
        a = [(OWN[i, j] + OWN[i, 4 - j]) / 2 for j in (0, 1)]
        b = [(OWN[i, j] - OWN[i, 4 - j]) / 2 for j in (0, 1)]
        p = (
            float(a[0]) * s0
            + float(a[1]) * s1
            + float(OWN[i, 2]) * m
            + float((HALF_L[i] + HALF_R[i]) / 2) * sp
        )
        q = float(b[0]) * d0 + float(b[1]) * d1 + float((HALF_L[i] - HALF_R[i]) / 2) * dp
        out[i] = p + q
        out[4 - i] = q - p
    b = [(OWN[2, j] - OWN[2, 4 - j]) / 2 for j in (0, 1)]
    out[2] = float(b[0]) * d0 + float(b[1]) * d1 + float((HALF_L[2] - HALF_R[2]) / 2) * dp
    return out


def modal_line(u):
    s0, s1, d0, d1, m = even_odd(u)
    out = []
    for k in range(5):
        if k % 2 == 0:
            out.append(
                float(MODAL[k, 0]) * s0 + float(MODAL[k, 1]) * s1 + float(MODAL[k, 2]) * m
            )
        else:
            out.append(float(MODAL[k, 0]) * d0 + float(MODAL[k, 1]) * d1)
    return out


def rows_roll(x, shift):
    return pltpu.roll(x, shift % 8, axis=x.ndim - 2)


def lanes_roll(x, shift):
    return pltpu.roll(x, shift % 128, axis=x.ndim - 1)


GROUPS = ((0, 2), (2, 4), (4, 5))
PAIRS = 63
ROUTES = {("u", 0): 0, ("u", 1): 1, ("u", 2): 2}
RELAYS = tuple(ROUTES)
SPOTS = tuple((dc, ds) for dc in (-1, 0, 1) for ds in (-1, 0, 1) if (dc, ds) != (0, 0))


def lift_rows():
    row = lax.broadcasted_iota(jnp.int32, (8, 128), 0)
    low_j = lax.rem(row, 2) == 0
    span = [jnp.where(low_j, float(HALF_L[b]), float(HALF_R[b])) for b in range(5)]
    chord = [
        jnp.where(row < 2, float(HALF_L[a]), jnp.where(row >= 6, float(HALF_R[a]), 0.0))
        for a in range(5)
    ]
    return span, chord


def kernel(
    chords,
    spans,
    x_hbm,
    r,
    vis,
    out_s,
    out_c,
    u,
    gs,
    gc,
    gn,
    modes,
    ts,
    tc,
    tsf,
    usr,
    usl,
    ucu,
    ucd,
    vsr,
    vsl,
    vcu,
    vcd,
    fsr,
    fsl,
    fcu,
    fcd,
    hsr,
    hsl,
    hcu,
    hcd,
    held,
    eps,
    eps_in,
    ks,
    kc,
    load_sem,
    e_send,
    e_recv,
    u_send,
    u_recv,
    f_send,
    f_recv,
    h_send,
    h_recv,
):
    c = lax.axis_index("chord")
    s = lax.axis_index("span")
    has_lo = c > 0
    has_hi = c < chords - 1
    s_of = {0: s, 1: lax.rem(s + 1, spans), -1: lax.rem(s + spans - 1, spans)}
    c_of = {0: c, 1: lax.rem(c + 1, chords), -1: lax.rem(c + chords - 1, chords)}

    def exists(dc):
        return {0: None, 1: has_hi, -1: has_lo}[dc]

    def guarded(cond, action):
        if cond is None:
            action()
        else:
            pl.when(cond)(action)

    loads = [pltpu.make_async_copy(x_hbm.at[v], u.at[v], load_sem.at[v]) for v in range(5)]
    for copy in loads:
        copy.start()

    barrier = pltpu.get_barrier_semaphore()
    for dc, ds in SPOTS:
        guarded(
            exists(dc),
            lambda dc=dc, ds=ds: pl.semaphore_signal(
                barrier, inc=1, device_id=(c_of[dc], s_of[ds]), device_id_type=MESH
            ),
        )

    half = chords // 2
    is_up = c == half - 1
    is_down = c == half
    stations = sorted(set(ROUTES.values()))

    def meet(cond, others):
        for other in others:
            pl.when(cond)(
                lambda other=other: pl.semaphore_signal(
                    barrier, inc=1, device_id=(other, s), device_id_type=MESH
                )
            )
        return jnp.where(cond, len(others), 0)

    last = chords - 1
    extra = 0
    for at, others in (
        (half - 1, [t for t in stations if t != half - 2] + [last - t for t in stations]),
        (half, [last - t for t in stations if t != half - 2] + [t for t in stations]),
    ):
        extra = extra + meet(c == at, others)
    for t in stations:
        near = [] if t == half - 2 else [half - 1]
        extra = extra + meet(c == t, near + [half])
        near = [] if t == half - 2 else [half]
        extra = extra + meet(c == last - t, near + [half - 1])

    row = lax.broadcasted_iota(jnp.int32, (8, 128), 0)
    lane = lax.broadcasted_iota(jnp.int32, (8, 128), 1)
    low_j = lax.rem(row, 2) == 0
    row_lo = row < 2
    row_hi = row >= 6
    first_lane = lane == 0
    last_lane = lane == 127

    def pick(mask, a, b):
        if a.ndim == 3:
            mask = jnp.broadcast_to(mask[None], a.shape)
        return jnp.where(mask, a, b)

    loads[0].wait()

    def modes_cb(a, carry):
        block = u[0, pl.ds(25 * a, 25)].reshape(5, 5, 8, 128)
        along_c = modal_line([block[:, k] for k in range(5)])
        stacked = [jnp.stack([along_c[o][b] for o in range(5)]) for b in range(5)]
        along_b = modal_line(stacked)
        for n in range(5):
            modes[pl.ds(25 * a + 5 * n, 5)] = along_b[n]
        return carry

    lax.fori_loop(0, 5, modes_cb, 0)
    low = jnp.zeros((4, 8, 128), jnp.float32)
    high = jnp.zeros((8, 128), jnp.float32)
    high4 = jnp.zeros((5, 8, 128), jnp.float32)
    for n in range(5):
        along_a = modal_line([modes[25 * a + 5 * n : 25 * a + 5 * n + 5] for a in range(5)])
        for m in range(5):
            square = along_a[m] * along_a[m]
            if n == 4 or m == 4:
                high4 = high4 + square
            else:
                low = low + square[:4]
                high = high + square[4]
    high = high + (high4[0] + high4[1]) + (high4[2] + high4[3]) + high4[4]
    total = (low[0] + low[1]) + (low[2] + low[3]) + high
    ratio = high / (total + ENERGY_EPS)
    level = jnp.log(jnp.maximum(ratio, RATIO_FLOOR)) * (1.0 / math.log(10.0))
    ramp = jnp.clip((level - SENSOR_CENTRE) / SENSOR_WIDTH, -1.0, 1.0)
    eps[...] = (EPS_SCALE * 0.5) * (1.0 + jnp.sin((0.5 * math.pi) * ramp))

    for v in range(1, 5):
        loads[v].wait()

    span_trace = [jnp.where(low_j, float(LEFT[b]), float(RIGHT[b])) for b in range(5)]
    chord_trace = [jnp.where(row_lo, float(LEFT[a]), float(RIGHT[a])) for a in range(5)]
    span_lift, chord_lift = lift_rows()

    def outer_traces(k, carry):
        v = k // 5
        i = k - 5 * v
        q = 25 * v + 5 * i
        acc = None
        for b in range(5):
            term = span_trace[b][None] * u[v, pl.ds(25 * i + 5 * b, 5)]
            acc = term if acc is None else acc + term
        ts[pl.ds(q, 5)] = acc
        acc = None
        for a in range(5):
            term = chord_trace[a][None] * u[v, pl.ds(25 * a + 5 * i, 5)]
            acc = term if acc is None else acc + term
        tc[pl.ds(q, 5)] = acc
        ucu[pl.ds(q, 5)] = acc[:, 6:8]
        ucd[pl.ds(q, 5)] = acc[:, 0:2]
        return carry

    lax.fori_loop(0, 25, outer_traces, 0)
    ts[125] = jnp.zeros((8, 128), jnp.float32)
    tsf[125] = jnp.zeros((8, 128), jnp.float32)

    def pack(src, to_right, to_left, first, count, step):
        def body(k, carry):
            p = first + step * k
            two = src[pl.ds(2 * p, 2 * step)].reshape(step, 2, 8, 128)
            one, other = two[:, 0], two[:, 1]
            to_right[pl.ds(p, step)] = pick(low_j, rows_roll(one, -1), other)
            to_left[pl.ds(p, step)] = pick(low_j, one, rows_roll(other, 1))
            return carry

        lax.fori_loop(0, count // step, body, 0)

    pack(ts, usr, usl, 0, PAIRS, 9)

    pl.semaphore_wait(barrier, 2 + jnp.where(has_lo, 3, 0) + jnp.where(has_hi, 3, 0) + extra)

    eps_copies = []
    for k, (dc, ds) in enumerate(SPOTS):
        copy = pltpu.make_async_remote_copy(
            src_ref=eps,
            dst_ref=eps_in.at[k],
            send_sem=e_send.at[k],
            recv_sem=e_recv.at[k],
            device_id=(c_of[dc], s_of[ds]),
            device_id_type=MESH,
        )
        guarded(exists(dc), copy.start)
        eps_copies.append((dc, ds, copy))

    def exchange(kind, g):
        (sr, sl, cu, cd), (dr, dl, du, dd), sems = messages[kind]
        v0, v1 = GROUPS[g]
        pairs = pl.ds(25 * v0 // 2, -(-25 * (v1 - v0) // 2))
        lines = pl.ds(25 * v0, 25 * (v1 - v0))
        out = []
        for k, (src, dst, dc, ds, part) in enumerate(
            (
                (sr, dr, 0, 1, pairs),
                (sl, dl, 0, -1, pairs),
                (cu, du, 1, 0, lines),
                (cd, dd, -1, 0, lines),
            )
        ):
            copy = pltpu.make_async_remote_copy(
                src_ref=src.at[part],
                dst_ref=dst.at[part],
                send_sem=sems[0].at[4 * g + k],
                recv_sem=sems[1].at[4 * g + k],
                device_id=(c_of[dc], s_of[ds]),
                device_id_type=MESH,
            )
            first = None
            if dc != 0 and (kind, g) in ROUTES:
                t = ROUTES[(kind, g)]
                n = RELAYS.index((kind, g))
                crossing = is_up if dc == 1 else is_down
                first = pltpu.make_async_remote_copy(
                    src_ref=src.at[part],
                    dst_ref=held.at[part],
                    send_sem=sems[0].at[4 * g + k],
                    recv_sem=h_recv.at[n],
                    device_id=(t if dc == 1 else last - t, s),
                    device_id_type=MESH,
                )
                second = pltpu.make_async_remote_copy(
                    src_ref=held.at[part],
                    dst_ref=dst.at[part],
                    send_sem=h_send.at[n],
                    recv_sem=sems[1].at[4 * g + k],
                    device_id=(half if dc == 1 else half - 1, s),
                    device_id_type=MESH,
                )
                first = (crossing, c == (t if dc == 1 else last - t), first, second)
            out.append((dc, copy, first))
        return out

    messages = {
        "u": ((usr, usl, ucu, ucd), (vsr, vsl, vcu, vcd), (u_send, u_recv)),
        "f": ((fsr, fsl, fcu, fcd), (hsr, hsl, hcu, hcd), (f_send, f_recv)),
    }
    u_copies = [exchange("u", g) for g in range(3)]
    f_copies = [exchange("f", g) for g in range(3)]

    def start(copies):
        for dc, copy, relay in copies:
            cond = exists(dc)
            if relay is not None:
                pl.when(relay[0])(relay[2].start)
                cond = jnp.logical_and(cond, jnp.logical_not(relay[0]))
            guarded(cond, copy.start)

    def pass_on(copies):
        for dc, copy, relay in copies:
            if relay is not None:

                def forward(relay=relay):
                    relay[2].wait_recv()
                    relay[3].start()

                pl.when(relay[1])(forward)

    def arrive(copies):
        for dc, copy, relay in copies:
            guarded(exists(-dc), copy.wait_recv)

    def sent(copies):
        for dc, copy, relay in copies:
            guarded(exists(dc), copy.wait_send)
            if relay is not None:
                pl.when(relay[1])(relay[3].wait_send)

    for g in range(3):
        start(u_copies[g])

    def local_ab(k, carry):
        v = k // 5
        a = k - 5 * v
        block = u[v, pl.ds(25 * a, 25)].reshape(5, 5, 8, 128)
        eo = even_odd([block[b] for b in range(5)])
        tl, tr = line_traces(eo)
        zero = jnp.zeros_like(tl)
        grad = line_apply(
            eo, pick(low_j, zero, rows_roll(tr, 1)), pick(low_j, rows_roll(tl, -1), zero)
        )
        for b in range(5):
            gs[v, pl.ds(25 * a + 5 * b, 5)] = grad[b]
        eo = even_odd([block[:, k] for k in range(5)])
        tl, tr = line_traces(eo)
        grad = line_apply(
            eo,
            pick(first_lane, tl, lanes_roll(tr, 1)),
            pick(last_lane, tr, lanes_roll(tl, -1)),
        )
        for b in range(5):
            gn[v, pl.ds(25 * a + 5 * b, 5)] = jnp.stack([grad[k][b] for k in range(5)])
        return carry

    lax.fori_loop(0, 25, local_ab, 0)

    def local_c(k, carry):
        v = k // 5
        b = k - 5 * v
        eo = even_odd([u[v, pl.ds(25 * a + 5 * b, 5)] for a in range(5)])
        tl, tr = line_traces(eo)
        zero = jnp.zeros_like(tl)
        grad = line_apply(
            eo, pick(row_lo, zero, rows_roll(tr, 2)), pick(row_hi, zero, rows_roll(tl, -2))
        )
        for a in range(5):
            gc[v, pl.ds(25 * a + 5 * b, 5)] = grad[a]
        return carry

    lax.fori_loop(0, 25, local_c, 0)
    for g in range(3):
        pass_on(u_copies[g])

    for dc, ds, copy in eps_copies:
        guarded(exists(-dc), copy.wait_recv)

    around = {(0, 0): eps[...]}
    for k, (dc, ds) in enumerate(SPOTS):
        value = eps_in[k]
        cond = exists(-dc)
        if cond is not None:
            value = jnp.where(cond, value, jnp.zeros_like(value))
        around[(-dc, -ds)] = value
    faces = {}
    for dc in (-1, 0, 1):
        mid, left, right = around[(dc, 0)], around[(dc, -1)], around[(dc, 1)]
        before = jnp.where(low_j, rows_roll(left, -1), rows_roll(mid, 1))
        after = jnp.where(low_j, rows_roll(mid, -1), rows_roll(right, 1))
        beyond = jnp.where(low_j, left, right)
        faces[dc] = (
            jnp.maximum(before, mid),
            jnp.maximum(mid, after),
            jnp.maximum(beyond, jnp.where(low_j, before, after)),
        )

    def normal_pair(x):
        zero = jnp.zeros_like(x)
        return (
            jnp.maximum(x, jnp.where(first_lane, zero, lanes_roll(x, 1))),
            jnp.maximum(x, jnp.where(last_lane, zero, lanes_roll(x, -1))),
        )

    corner = {}
    span_far = {}
    chord_far = {}
    for k in range(3):
        below, mid, above = faces[-1][k], faces[0][k], faces[1][k]
        before = jnp.where(row_lo, rows_roll(below, 2), rows_roll(mid, 2))
        after = jnp.where(row_hi, rows_roll(above, -2), rows_roll(mid, -2))
        for sx, value in ((0, jnp.maximum(before, mid)), (1, jnp.maximum(mid, after))):
            pair = normal_pair(value)
            for sz in range(2):
                if k == 2:
                    span_far[(sx, sz)] = pair[sz]
                else:
                    corner[(sx, k, sz)] = pair[sz]
        if k < 2:
            beyond = jnp.where(row_lo, rows_roll(below, 4), rows_roll(above, 4))
            pair = normal_pair(jnp.maximum(beyond, jnp.where(row_lo, before, after)))
            for sz in range(2):
                chord_far[(k, sz)] = pair[sz]

    def between(lo, hi):
        step = hi - lo
        return [lo + float(UPPER[i]) * step for i in range(5)]

    plane = {
        (sy, sz): between(corner[(0, sy, sz)], corner[(1, sy, sz)])
        for sy in range(2)
        for sz in range(2)
    }
    for a in range(5):
        edge = [between(plane[(0, sz)][a], plane[(1, sz)][a]) for sz in range(2)]
        for b in range(5):
            vis[pl.ds(25 * a + 5 * b, 5)] = jnp.stack(between(edge[0][b], edge[1][b]))
    weight = {}
    for sx in range(2):
        for sz in range(2):
            near = jnp.where(low_j, corner[(sx, 0, sz)], corner[(sx, 1, sz)])
            value = K_FAR * span_far[(sx, sz)] + K_NEAR * near
            weight[(sx, sz)] = jnp.where(low_j, value, -value)
    edge = [between(weight[(0, sz)], weight[(1, sz)]) for sz in range(2)]
    for a in range(5):
        ks[pl.ds(5 * a, 5)] = jnp.stack(between(edge[0][a], edge[1][a]))
    for sy in range(2):
        for sz in range(2):
            near = jnp.where(row_lo, corner[(0, sy, sz)], corner[(1, sy, sz)])
            value = K_FAR * chord_far[(sy, sz)] + K_NEAR * near
            weight[(sy, sz)] = jnp.where(row_lo, value, -value)
    edge = [between(weight[(0, sz)], weight[(1, sz)]) for sz in range(2)]
    for b in range(5):
        kc[pl.ds(5 * b, 5)] = jnp.stack(between(edge[0][b], edge[1][b]))

    def flux_traces(k, carry):
        v = k // 5
        a = k - 5 * v
        at = [pl.ds(25 * a + 5 * b, 5) for b in range(5)]
        acc = None
        for b in range(5):
            term = span_trace[b][None] * (vis[at[b]] * gs[v, at[b]])
            acc = term if acc is None else acc + term
        tsf[pl.ds(25 * v + 5 * a, 5)] = acc
        at = [pl.ds(25 * i + 5 * a, 5) for i in range(5)]
        acc = None
        for i in range(5):
            term = chord_trace[i][None] * (vis[at[i]] * gc[v, at[i]])
            acc = term if acc is None else acc + term
        q = 25 * v + 5 * a
        fcu[pl.ds(q, 5)] = acc[:, 6:8]
        fcd[pl.ds(q, 5)] = acc[:, 0:2]
        return carry

    for g, (v0, v1) in enumerate(GROUPS):
        lax.fori_loop(5 * v0, 5 * v1, flux_traces, 0)
        count = -(-25 * (v1 - v0) // 2)
        pack(tsf, fsr, fsl, 25 * v0 // 2, count, 5 if count % 5 == 0 else count)
        start(f_copies[g])

    def normal_part(k, carry):
        v = k // 5
        a = k - 5 * v
        block = gn[v, pl.ds(25 * a, 25)] * vis[pl.ds(25 * a, 25)]
        block = block.reshape(5, 5, 8, 128)
        eo = even_odd([block[:, i] for i in range(5)])
        tl, tr = line_traces(eo)
        out = line_apply(
            eo,
            pick(first_lane, -tl, lanes_roll(tr, 1)),
            pick(last_lane, -tr, lanes_roll(tl, -1)),
        )
        for b in range(5):
            r[v, pl.ds(25 * a + 5 * b, 5)] = jnp.stack([out[i][b] for i in range(5)])
        return carry

    lax.fori_loop(0, 25, normal_part, 0)

    end_lo = jnp.logical_and(row_lo, jnp.logical_not(has_lo))
    end_hi = jnp.logical_and(row_hi, jnp.logical_not(has_hi))

    def unpack(from_left, from_right, dst, first, count, step):
        def body(k, carry):
            p = first + step * k
            a, b = from_left[pl.ds(p, step)], from_right[pl.ds(p, step)]
            one = pick(low_j, a, rows_roll(b, 1))
            other = pick(low_j, rows_roll(a, -1), b)
            dst[pl.ds(2 * p, 2 * step)] = jnp.stack([one, other], axis=1).reshape(
                2 * step, 8, 128
            )
            return carry

        lax.fori_loop(0, count // step, body, 0)

    def chord_outer(from_lo, from_hi, q):
        lo = from_lo[pl.ds(q, 5)]
        hi = from_hi[pl.ds(q, 5)]
        gap = jnp.zeros((5, 4, 128), jnp.float32)
        return jnp.concatenate([lo, gap, hi], axis=1)

    def span_part(k, carry):
        v = k // 5
        a = k - 5 * v
        outer = tsf[pl.ds(25 * v + 5 * a, 5)]
        flux = [
            vis[pl.ds(25 * a + 5 * b, 5)]
            * (gs[v, pl.ds(25 * a + 5 * b, 5)] + span_lift[b][None] * outer)
            for b in range(5)
        ]
        eo = even_odd(flux)
        tl, tr = line_traces(eo)
        zero = jnp.zeros_like(tl)
        out = line_apply(
            eo, pick(low_j, zero, rows_roll(tr, 1)), pick(low_j, rows_roll(tl, -1), zero)
        )
        for b in range(5):
            at = pl.ds(25 * a + 5 * b, 5)
            r[v, at] = r[v, at] + out[b]
        return carry

    def chord_part(k, carry):
        v = k // 5
        b = k - 5 * v
        q = 25 * v + 5 * b
        own = tc[pl.ds(q, 5)]
        outer = chord_outer(vcu, vcd, q)
        outer = pick(jnp.logical_or(end_lo, end_hi), own, outer)
        flux = [
            vis[pl.ds(25 * a + 5 * b, 5)]
            * (gc[v, pl.ds(25 * a + 5 * b, 5)] + chord_lift[a][None] * outer)
            for a in range(5)
        ]
        eo = even_odd(flux)
        tl, tr = line_traces(eo)
        zero = jnp.zeros_like(tl)
        out = line_apply(
            eo,
            pick(row_lo, pick(end_lo, -tl, zero), rows_roll(tr, 2)),
            pick(row_hi, pick(end_hi, -tr, zero), rows_roll(tl, -2)),
        )
        for a in range(5):
            at = pl.ds(25 * a + 5 * b, 5)
            r[v, at] = r[v, at] + out[a]
        return carry

    for g, (v0, v1) in enumerate(GROUPS):
        arrive(u_copies[g])
        count = -(-25 * (v1 - v0) // 2)
        unpack(vsr, vsl, tsf, 25 * v0 // 2, count, 5 if count % 5 == 0 else count)
        lax.fori_loop(5 * v0, 5 * v1, span_part, 0)
        lax.fori_loop(5 * v0, 5 * v1, chord_part, 0)
        pass_on(f_copies[g])

    def span_outer(q, at):
        return tsf[pl.ds(q, 5)] + ks[pl.ds(at, 5)] * ts[pl.ds(q, 5)]

    def chord_flux(q, at):
        outer = chord_outer(hcu, hcd, q) + kc[pl.ds(at, 5)] * tc[pl.ds(q, 5)]
        return pick(jnp.logical_or(end_lo, end_hi), jnp.zeros_like(outer), outer)

    def finish(k, carry):
        v = k // 5
        a = k - 5 * v
        outer = span_outer(25 * v + 5 * a, 5 * a)
        for b in range(5):
            at = pl.ds(25 * a + 5 * b, 5)
            r[v, at] = r[v, at] + span_lift[b][None] * outer
        return carry

    def finish_chord(k, carry):
        v = k // 5
        b = k - 5 * v
        outer = chord_flux(25 * v + 5 * b, 5 * b)
        for a in range(5):
            at = pl.ds(25 * a + 5 * b, 5)
            r[v, at] = r[v, at] + chord_lift[a][None] * outer
        return carry

    for g, (v0, v1) in enumerate(GROUPS):
        arrive(f_copies[g])
        count = -(-25 * (v1 - v0) // 2)
        unpack(hsr, hsl, tsf, 25 * v0 // 2, count, 5 if count % 5 == 0 else count)
        if g < 2:
            lax.fori_loop(5 * v0, 5 * v1, finish, 0)
            lax.fori_loop(5 * v0, 5 * v1, finish_chord, 0)
        else:
            for k in range(5):
                at = pl.ds(5 * k, 5)
                out_s[at] = span_outer(100 + 5 * k, 5 * k)
                out_c[at] = chord_flux(100 + 5 * k, 5 * k)
    for dc, ds, copy in eps_copies:
        guarded(exists(dc), copy.wait_send)
    for g in range(3):
        sent(u_copies[g])
        sent(f_copies[g])


def store_kernel(r, vis, out_s, out_c, res_hbm, vis_hbm, final, sem):
    copies = [pltpu.make_async_copy(r.at[v], res_hbm.at[v], sem.at[v]) for v in range(4)]
    copies.append(pltpu.make_async_copy(vis, vis_hbm, sem.at[5]))
    for copy in copies:
        copy.start()
    span, chord = lift_rows()
    for a in range(5):
        for b in range(5):
            at = pl.ds(25 * a + 5 * b, 5)
            final[at] = (
                r[4, at]
                + span[b][None] * out_s[pl.ds(5 * a, 5)]
                + chord[a][None] * out_c[pl.ds(5 * b, 5)]
            )
    copies.append(pltpu.make_async_copy(final, res_hbm.at[4], sem.at[4]))
    copies[-1].start()
    for copy in copies:
        copy.wait()


def shards(state):
    chords, spans = lax.axis_size("chord"), lax.axis_size("span")
    f32 = jnp.float32
    field = pltpu.VMEM((5, 125, 8, 128), f32)
    pairs = pltpu.VMEM((PAIRS, 8, 128), f32)
    thin = pltpu.VMEM((132, 2, 128), f32)
    sem = pltpu.SemaphoreType.DMA
    partial, viscosity, out_s, out_c = pl.pallas_call(
        functools.partial(kernel, chords, spans),
        out_shape=(
            jax.ShapeDtypeStruct((5, 125, 8, 128), f32),
            jax.ShapeDtypeStruct((125, 8, 128), f32),
            jax.ShapeDtypeStruct((25, 8, 128), f32),
            jax.ShapeDtypeStruct((25, 8, 128), f32),
        ),
        in_specs=[pl.BlockSpec(memory_space=pltpu.HBM)],
        out_specs=(pl.BlockSpec(memory_space=pltpu.VMEM),) * 4,
        scratch_shapes=[
            field,
            field,
            field,
            field,
            pltpu.VMEM((125, 8, 128), f32),
            pltpu.VMEM((126, 8, 128), f32),
            pltpu.VMEM((125, 8, 128), f32),
            pltpu.VMEM((126, 8, 128), f32),
        ]
        + [pairs, pairs, thin, thin] * 4
        + [thin]
        + [
            pltpu.VMEM((8, 128), f32),
            pltpu.VMEM((8, 8, 128), f32),
            pltpu.VMEM((25, 8, 128), f32),
            pltpu.VMEM((25, 8, 128), f32),
            sem((5,)),
            sem((8,)),
            sem((8,)),
            sem((12,)),
            sem((12,)),
            sem((12,)),
            sem((12,)),
            sem((len(RELAYS),)),
            sem((len(RELAYS),)),
        ],
        compiler_params=pltpu.CompilerParams(
            collective_id=0, has_side_effects=True, vmem_limit_bytes=40 * 1024 * 1024
        ),
        name="viscous",
    )(pltpu.with_memory_space_constraint(state.reshape(5, 125, 8, 128), pltpu.HBM))
    residual, viscosity = pl.pallas_call(
        store_kernel,
        out_shape=(
            jax.ShapeDtypeStruct((5, 125, 8, 128), f32),
            jax.ShapeDtypeStruct((125, 8, 128), f32),
        ),
        in_specs=[pl.BlockSpec(memory_space=pltpu.VMEM)] * 4,
        out_specs=(pl.BlockSpec(memory_space=pl.ANY), pl.BlockSpec(memory_space=pl.ANY)),
        scratch_shapes=[pltpu.VMEM((125, 8, 128), f32), sem((6,))],
        compiler_params=pltpu.CompilerParams(vmem_limit_bytes=4 * 1024 * 1024),
        name="store",
    )(partial, viscosity, out_s, out_c)
    return residual.reshape(state.shape), viscosity.reshape(state.shape[1:])


def solution(mesh):
    in_specs = (P(None, None, "chord", "span", None),)
    out_specs = (P(None, None, "chord", "span", None), P(None, "chord", "span", None))
    return jax.shard_map(shards, mesh=mesh, in_specs=in_specs, out_specs=out_specs, check_vma=False)
```

```python
import functools
import math

import jax
import jax.numpy as jnp
import numpy as np
from jax import lax
from jax.experimental import pallas as pl
from jax.experimental.pallas import tpu as pltpu
from jax.sharding import PartitionSpec as P

MESH = pl.DeviceIdType.MESH
EPS_SCALE = 0.01
SENSOR_CENTRE = -3.0
SENSOR_WIDTH = 1.5
RATIO_FLOOR = 1e-06
ENERGY_EPS = 1e-06
NODES = [-0.906179845938664, -0.5384693101056831, 0.0, 0.5384693101056831, 0.906179845938664]
WEIGHTS = [
    0.2369268850561891,
    0.4786286704993665,
    0.5688888888888889,
    0.4786286704993665,
    0.2369268850561891,
]


def legendre_values(points):
    values = [np.ones(points.shape), np.array(points)]
    for order in range(1, 5):
        values.append(
            ((2 * order + 1) * points * values[order] - order * values[order - 1]) / (order + 1)
        )
    return values


def tables():
    x = np.array(NODES)
    w = np.array(WEIGHTS)
    bary = np.array([1.0 / np.prod([x[j] - x[k] for k in range(5) if k != j]) for j in range(5)])
    deriv = np.zeros((5, 5))
    for i in range(5):
        for j in range(5):
            if i != j:
                deriv[i, j] = bary[j] / bary[i] / (x[i] - x[j])
        deriv[i, i] = -np.sum(deriv[i])
    left = np.ones(5)
    right = np.ones(5)
    for j in range(5):
        for k in range(5):
            if k != j:
                left[j] *= (-1.0 - x[k]) / (x[j] - x[k])
                right[j] *= (1.0 - x[k]) / (x[j] - x[k])
    legendre = legendre_values(x)
    fourth = 7.0 * legendre[3] + 3.0 * legendre[1]
    fifth = 9.0 * legendre[4] + 5.0 * legendre[2] + legendre[0]
    half_l = 0.25 * (fourth - fifth)
    half_r = 0.25 * (fourth + fifth)
    modal = np.zeros((5, 5))
    for k in range(5):
        modal[k, :] = w * math.sqrt((2 * k + 1) / 2.0) * legendre[k]
    own = deriv - np.outer(half_l, left) - np.outer(half_r, right)
    upper = (1.0 + x) / 2.0
    near = float(np.sum(right * half_r * upper))
    far = float(np.sum(right * half_r * (1.0 - upper)))
    return own, left, right, half_l, half_r, modal, upper, near, far


OWN, LEFT, RIGHT, HALF_L, HALF_R, MODAL, UPPER, K_NEAR, K_FAR = tables()


def even_odd(u):
    return u[0] + u[4], u[1] + u[3], u[0] - u[4], u[1] - u[3], u[2]


def line_traces(eo):
    s0, s1, d0, d1, m = eo
    even = (
        float((RIGHT[0] + RIGHT[4]) / 2) * s0
        + float((RIGHT[1] + RIGHT[3]) / 2) * s1
        + float(RIGHT[2]) * m
    )
    odd = float((RIGHT[0] - RIGHT[4]) / 2) * d0 + float((RIGHT[1] - RIGHT[3]) / 2) * d1
    return even - odd, even + odd


def line_apply(eo, prev, following):
    s0, s1, d0, d1, m = eo
    sp = prev + following
    dp = prev - following
    out = [None] * 5
    for i in (0, 1):
        a = [(OWN[i, j] + OWN[i, 4 - j]) / 2 for j in (0, 1)]
        b = [(OWN[i, j] - OWN[i, 4 - j]) / 2 for j in (0, 1)]
        p = (
            float(a[0]) * s0
            + float(a[1]) * s1
            + float(OWN[i, 2]) * m
            + float((HALF_L[i] + HALF_R[i]) / 2) * sp
        )
        q = float(b[0]) * d0 + float(b[1]) * d1 + float((HALF_L[i] - HALF_R[i]) / 2) * dp
        out[i] = p + q
        out[4 - i] = q - p
    b = [(OWN[2, j] - OWN[2, 4 - j]) / 2 for j in (0, 1)]
    out[2] = float(b[0]) * d0 + float(b[1]) * d1 + float((HALF_L[2] - HALF_R[2]) / 2) * dp
    return out


def modal_line(u):
    s0, s1, d0, d1, m = even_odd(u)
    out = []
    for k in range(5):
        if k % 2 == 0:
            out.append(
                float(MODAL[k, 0]) * s0 + float(MODAL[k, 1]) * s1 + float(MODAL[k, 2]) * m
            )
        else:
            out.append(float(MODAL[k, 0]) * d0 + float(MODAL[k, 1]) * d1)
    return out


def rows_roll(x, shift):
    return pltpu.roll(x, shift % 8, axis=x.ndim - 2)


def lanes_roll(x, shift):
    return pltpu.roll(x, shift % 128, axis=x.ndim - 1)


GROUPS = ((0, 2), (2, 4), (4, 5))
PAIRS = 63
PAD = 4
ROUTES = {("u", 0): 0, ("u", 1): 1, ("u", 2): 2}
RELAYS = tuple(ROUTES)
SPOTS = tuple((dc, ds) for dc in (-1, 0, 1) for ds in (-1, 0, 1) if (dc, ds) != (0, 0))


def lift_rows():
    row = lax.broadcasted_iota(jnp.int32, (8, 128), 0)
    low_j = lax.rem(row, 2) == 0
    span = [jnp.where(low_j, float(HALF_L[b]), float(HALF_R[b])) for b in range(5)]
    chord = [
        jnp.where(row < 2, float(HALF_L[a]), jnp.where(row >= 6, float(HALF_R[a]), 0.0))
        for a in range(5)
    ]
    return span, chord


def kernel(
    chords,
    spans,
    x_hbm,
    r,
    vis,
    out_s,
    out_c,
    u,
    gs,
    gc,
    gn,
    modes,
    ts,
    tc,
    tsf,
    usr,
    usl,
    ucu,
    ucd,
    vsr,
    vsl,
    vcu,
    vcd,
    fsr,
    fsl,
    fcu,
    fcd,
    hsr,
    hsl,
    hcu,
    hcd,
    held,
    eps,
    eps_in,
    ks,
    kc,
    load_sem,
    e_send,
    e_recv,
    u_send,
    u_recv,
    f_send,
    f_recv,
    h_send,
    h_recv,
):
    c = lax.axis_index("chord")
    s = lax.axis_index("span")
    has_lo = c > 0
    has_hi = c < chords - 1
    s_of = {0: s, 1: lax.rem(s + 1, spans), -1: lax.rem(s + spans - 1, spans)}
    c_of = {0: c, 1: lax.rem(c + 1, chords), -1: lax.rem(c + chords - 1, chords)}

    def exists(dc):
        return {0: None, 1: has_hi, -1: has_lo}[dc]

    def guarded(cond, action):
        if cond is None:
            action()
        else:
            pl.when(cond)(action)

    loads = [pltpu.make_async_copy(x_hbm.at[v], u.at[v], load_sem.at[v]) for v in range(5)]
    for copy in loads:
        copy.start()

    barrier = pltpu.get_barrier_semaphore()
    for dc, ds in SPOTS:
        guarded(
            exists(dc),
            lambda dc=dc, ds=ds: pl.semaphore_signal(
                barrier, inc=1, device_id=(c_of[dc], s_of[ds]), device_id_type=MESH
            ),
        )

    half = chords // 2
    is_up = c == half - 1
    is_down = c == half
    stations = sorted(set(ROUTES.values()))

    def meet(cond, others):
        for other in others:
            pl.when(cond)(
                lambda other=other: pl.semaphore_signal(
                    barrier, inc=1, device_id=(other, s), device_id_type=MESH
                )
            )
        return jnp.where(cond, len(others), 0)

    last = chords - 1
    extra = 0
    for at, others in (
        (half - 1, [t for t in stations if t != half - 2] + [last - t for t in stations]),
        (half, [last - t for t in stations if t != half - 2] + [t for t in stations]),
    ):
        extra = extra + meet(c == at, others)
    for t in stations:
        near = [] if t == half - 2 else [half - 1]
        extra = extra + meet(c == t, near + [half])
        near = [] if t == half - 2 else [half]
        extra = extra + meet(c == last - t, near + [half - 1])

    row = lax.broadcasted_iota(jnp.int32, (8, 128), 0)
    lane = lax.broadcasted_iota(jnp.int32, (8, 128), 1)
    low_j = lax.rem(row, 2) == 0
    row_lo = row < 2
    row_hi = row >= 6
    first_lane = lane == 0
    last_lane = lane == 127

    def pick(mask, a, b):
        if a.ndim == 3:
            mask = jnp.broadcast_to(mask[None], a.shape)
        return jnp.where(mask, a, b)

    loads[0].wait()

    def modes_cb(a, carry):
        block = u[0, pl.ds(25 * a, 25)].reshape(5, 5, 8, 128)
        along_c = modal_line([block[:, k] for k in range(5)])
        stacked = [jnp.stack([along_c[o][b] for o in range(5)]) for b in range(5)]
        along_b = modal_line(stacked)
        for n in range(5):
            modes[pl.ds(25 * a + 5 * n, 5)] = along_b[n]
        return carry

    lax.fori_loop(0, 5, modes_cb, 0)
    low = jnp.zeros((4, 8, 128), jnp.float32)
    high = jnp.zeros((8, 128), jnp.float32)
    high4 = jnp.zeros((5, 8, 128), jnp.float32)
    for n in range(5):
        along_a = modal_line([modes[25 * a + 5 * n : 25 * a + 5 * n + 5] for a in range(5)])
        for m in range(5):
            square = along_a[m] * along_a[m]
            if n == 4 or m == 4:
                high4 = high4 + square
            else:
                low = low + square[:4]
                high = high + square[4]
    high = high + (high4[0] + high4[1]) + (high4[2] + high4[3]) + high4[4]
    total = (low[0] + low[1]) + (low[2] + low[3]) + high
    ratio = high / (total + ENERGY_EPS)
    level = jnp.log(jnp.maximum(ratio, RATIO_FLOOR)) * (1.0 / math.log(10.0))
    ramp = jnp.clip((level - SENSOR_CENTRE) / SENSOR_WIDTH, -1.0, 1.0)
    eps[...] = (EPS_SCALE * 0.5) * (1.0 + jnp.sin((0.5 * math.pi) * ramp))

    for v in range(1, 5):
        loads[v].wait()

    span_trace = [jnp.where(low_j, float(LEFT[b]), float(RIGHT[b])) for b in range(5)]
    chord_trace = [jnp.where(row_lo, float(LEFT[a]), float(RIGHT[a])) for a in range(5)]
    span_lift, chord_lift = lift_rows()

    def outer_traces(k, carry):
        v = k // 5
        i = k - 5 * v
        q = 25 * v + 5 * i
        acc = None
        for b in range(5):
            term = span_trace[b][None] * u[v, pl.ds(25 * i + 5 * b, 5)]
            acc = term if acc is None else acc + term
        ts[pl.ds(q, 5)] = acc
        acc = None
        for a in range(5):
            term = chord_trace[a][None] * u[v, pl.ds(25 * a + 5 * i, 5)]
            acc = term if acc is None else acc + term
        tc[pl.ds(q, 5)] = acc
        ucu[pl.ds(PAD + q, 5)] = rows_roll(acc, 2)[:, 0:2]
        ucd[pl.ds(PAD + q, 5)] = acc[:, 0:2]
        return carry

    lax.fori_loop(0, 25, outer_traces, 0)
    ts[125] = jnp.zeros((8, 128), jnp.float32)
    tsf[125] = jnp.zeros((8, 128), jnp.float32)

    def pack(src, to_right, to_left, first, count, step):
        def body(k, carry):
            p = first + step * k
            two = src[pl.ds(2 * p, 2 * step)].reshape(step, 2, 8, 128)
            one, other = two[:, 0], two[:, 1]
            to_right[pl.ds(p, step)] = pick(low_j, rows_roll(one, -1), other)
            to_left[pl.ds(p, step)] = pick(low_j, one, rows_roll(other, 1))
            return carry

        lax.fori_loop(0, count // step, body, 0)

    pack(ts, usr, usl, 0, PAIRS, 9)

    pl.semaphore_wait(barrier, 2 + jnp.where(has_lo, 3, 0) + jnp.where(has_hi, 3, 0) + extra)

    eps_copies = []
    for k, (dc, ds) in enumerate(SPOTS):
        copy = pltpu.make_async_remote_copy(
            src_ref=eps,
            dst_ref=eps_in.at[k],
            send_sem=e_send.at[k],
            recv_sem=e_recv.at[k],
            device_id=(c_of[dc], s_of[ds]),
            device_id_type=MESH,
        )
        guarded(exists(dc), copy.start)
        eps_copies.append((dc, ds, copy))

    def exchange(kind, g):
        (sr, sl, cu, cd), (dr, dl, du, dd), sems = messages[kind]
        v0, v1 = GROUPS[g]
        pairs = pl.ds(25 * v0 // 2, -(-25 * (v1 - v0) // 2))
        lines = pl.ds(PAD + 25 * v0, 25 * (v1 - v0))
        out = []
        for k, (src, dst, dc, ds, part) in enumerate(
            (
                (sr, dr, 0, 1, pairs),
                (sl, dl, 0, -1, pairs),
                (cu, du, 1, 0, lines),
                (cd, dd, -1, 0, lines),
            )
        ):
            copy = pltpu.make_async_remote_copy(
                src_ref=src.at[part],
                dst_ref=dst.at[part],
                send_sem=sems[0].at[4 * g + k],
                recv_sem=sems[1].at[4 * g + k],
                device_id=(c_of[dc], s_of[ds]),
                device_id_type=MESH,
            )
            first = None
            if dc != 0 and (kind, g) in ROUTES:
                t = ROUTES[(kind, g)]
                n = RELAYS.index((kind, g))
                crossing = is_up if dc == 1 else is_down
                first = pltpu.make_async_remote_copy(
                    src_ref=src.at[part],
                    dst_ref=held.at[part],
                    send_sem=sems[0].at[4 * g + k],
                    recv_sem=h_recv.at[n],
                    device_id=(t if dc == 1 else last - t, s),
                    device_id_type=MESH,
                )
                second = pltpu.make_async_remote_copy(
                    src_ref=held.at[part],
                    dst_ref=dst.at[part],
                    send_sem=h_send.at[n],
                    recv_sem=sems[1].at[4 * g + k],
                    device_id=(half if dc == 1 else half - 1, s),
                    device_id_type=MESH,
                )
                first = (crossing, c == (t if dc == 1 else last - t), first, second)
            out.append((dc, copy, first))
        return out

    messages = {
        "u": ((usr, usl, ucu, ucd), (vsr, vsl, vcu, vcd), (u_send, u_recv)),
        "f": ((fsr, fsl, fcu, fcd), (hsr, hsl, hcu, hcd), (f_send, f_recv)),
    }
    u_copies = [exchange("u", g) for g in range(3)]
    f_copies = [exchange("f", g) for g in range(3)]

    def start(copies):
        for dc, copy, relay in copies:
            cond = exists(dc)
            if relay is not None:
                pl.when(relay[0])(relay[2].start)
                cond = jnp.logical_and(cond, jnp.logical_not(relay[0]))
            guarded(cond, copy.start)

    def pass_on(copies):
        for dc, copy, relay in copies:
            if relay is not None:

                def forward(relay=relay):
                    relay[2].wait_recv()
                    relay[3].start()

                pl.when(relay[1])(forward)

    def arrive(copies):
        for dc, copy, relay in copies:
            guarded(exists(-dc), copy.wait_recv)

    def sent(copies):
        for dc, copy, relay in copies:
            guarded(exists(dc), copy.wait_send)
            if relay is not None:
                pl.when(relay[1])(relay[3].wait_send)

    for g in range(3):
        start(u_copies[g])

    def local_ab(k, carry):
        v = k // 5
        a = k - 5 * v
        block = u[v, pl.ds(25 * a, 25)].reshape(5, 5, 8, 128)
        eo = even_odd([block[b] for b in range(5)])
        tl, tr = line_traces(eo)
        zero = jnp.zeros_like(tl)
        grad = line_apply(
            eo, pick(low_j, zero, rows_roll(tr, 1)), pick(low_j, rows_roll(tl, -1), zero)
        )
        for b in range(5):
            gs[v, pl.ds(25 * a + 5 * b, 5)] = grad[b]
        eo = even_odd([block[:, k] for k in range(5)])
        tl, tr = line_traces(eo)
        grad = line_apply(
            eo,
            pick(first_lane, tl, lanes_roll(tr, 1)),
            pick(last_lane, tr, lanes_roll(tl, -1)),
        )
        for b in range(5):
            gn[v, pl.ds(25 * a + 5 * b, 5)] = jnp.stack([grad[k][b] for k in range(5)])
        return carry

    lax.fori_loop(0, 25, local_ab, 0)

    def local_c(k, carry):
        v = k // 5
        b = k - 5 * v
        eo = even_odd([u[v, pl.ds(25 * a + 5 * b, 5)] for a in range(5)])
        tl, tr = line_traces(eo)
        zero = jnp.zeros_like(tl)
        grad = line_apply(
            eo, pick(row_lo, zero, rows_roll(tr, 2)), pick(row_hi, zero, rows_roll(tl, -2))
        )
        for a in range(5):
            gc[v, pl.ds(25 * a + 5 * b, 5)] = grad[a]
        return carry

    lax.fori_loop(0, 25, local_c, 0)
    for g in range(3):
        pass_on(u_copies[g])

    for dc, ds, copy in eps_copies:
        guarded(exists(-dc), copy.wait_recv)

    around = {(0, 0): eps[...]}
    for k, (dc, ds) in enumerate(SPOTS):
        value = eps_in[k]
        cond = exists(-dc)
        if cond is not None:
            value = jnp.where(cond, value, jnp.zeros_like(value))
        around[(-dc, -ds)] = value
    faces = {}
    for dc in (-1, 0, 1):
        mid, left, right = around[(dc, 0)], around[(dc, -1)], around[(dc, 1)]
        before = jnp.where(low_j, rows_roll(left, -1), rows_roll(mid, 1))
        after = jnp.where(low_j, rows_roll(mid, -1), rows_roll(right, 1))
        beyond = jnp.where(low_j, left, right)
        faces[dc] = (
            jnp.maximum(before, mid),
            jnp.maximum(mid, after),
            jnp.maximum(beyond, jnp.where(low_j, before, after)),
        )

    def normal_pair(x):
        zero = jnp.zeros_like(x)
        return (
            jnp.maximum(x, jnp.where(first_lane, zero, lanes_roll(x, 1))),
            jnp.maximum(x, jnp.where(last_lane, zero, lanes_roll(x, -1))),
        )

    corner = {}
    span_far = {}
    chord_far = {}
    for k in range(3):
        below, mid, above = faces[-1][k], faces[0][k], faces[1][k]
        before = jnp.where(row_lo, rows_roll(below, 2), rows_roll(mid, 2))
        after = jnp.where(row_hi, rows_roll(above, -2), rows_roll(mid, -2))
        for sx, value in ((0, jnp.maximum(before, mid)), (1, jnp.maximum(mid, after))):
            pair = normal_pair(value)
            for sz in range(2):
                if k == 2:
                    span_far[(sx, sz)] = pair[sz]
                else:
                    corner[(sx, k, sz)] = pair[sz]
        if k < 2:
            beyond = jnp.where(row_lo, rows_roll(below, 4), rows_roll(above, 4))
            pair = normal_pair(jnp.maximum(beyond, jnp.where(row_lo, before, after)))
            for sz in range(2):
                chord_far[(k, sz)] = pair[sz]

    def between(lo, hi):
        step = hi - lo
        return [lo + float(UPPER[i]) * step for i in range(5)]

    plane = {
        (sy, sz): between(corner[(0, sy, sz)], corner[(1, sy, sz)])
        for sy in range(2)
        for sz in range(2)
    }
    for a in range(5):
        edge = [between(plane[(0, sz)][a], plane[(1, sz)][a]) for sz in range(2)]
        for b in range(5):
            vis[pl.ds(25 * a + 5 * b, 5)] = jnp.stack(between(edge[0][b], edge[1][b]))
    weight = {}
    for sx in range(2):
        for sz in range(2):
            near = jnp.where(low_j, corner[(sx, 0, sz)], corner[(sx, 1, sz)])
            value = K_FAR * span_far[(sx, sz)] + K_NEAR * near
            weight[(sx, sz)] = jnp.where(low_j, value, -value)
    edge = [between(weight[(0, sz)], weight[(1, sz)]) for sz in range(2)]
    for a in range(5):
        ks[pl.ds(5 * a, 5)] = jnp.stack(between(edge[0][a], edge[1][a]))
    for sy in range(2):
        for sz in range(2):
            near = jnp.where(row_lo, corner[(0, sy, sz)], corner[(1, sy, sz)])
            value = K_FAR * chord_far[(sy, sz)] + K_NEAR * near
            weight[(sy, sz)] = jnp.where(row_lo, value, -value)
    edge = [between(weight[(0, sz)], weight[(1, sz)]) for sz in range(2)]
    for b in range(5):
        kc[pl.ds(5 * b, 5)] = jnp.stack(between(edge[0][b], edge[1][b]))

    def flux_traces(k, carry):
        v = k // 5
        a = k - 5 * v
        at = [pl.ds(25 * a + 5 * b, 5) for b in range(5)]
        acc = None
        for b in range(5):
            term = span_trace[b][None] * (vis[at[b]] * gs[v, at[b]])
            acc = term if acc is None else acc + term
        tsf[pl.ds(25 * v + 5 * a, 5)] = acc
        at = [pl.ds(25 * i + 5 * a, 5) for i in range(5)]
        acc = None
        for i in range(5):
            term = chord_trace[i][None] * (vis[at[i]] * gc[v, at[i]])
            acc = term if acc is None else acc + term
        q = 25 * v + 5 * a
        fcu[pl.ds(PAD + q, 5)] = rows_roll(acc, 2)[:, 0:2]
        fcd[pl.ds(PAD + q, 5)] = acc[:, 0:2]
        return carry

    for g, (v0, v1) in enumerate(GROUPS):
        lax.fori_loop(5 * v0, 5 * v1, flux_traces, 0)
        count = -(-25 * (v1 - v0) // 2)
        pack(tsf, fsr, fsl, 25 * v0 // 2, count, 5 if count % 5 == 0 else count)
        start(f_copies[g])

    def normal_part(k, carry):
        v = k // 5
        a = k - 5 * v
        block = gn[v, pl.ds(25 * a, 25)] * vis[pl.ds(25 * a, 25)]
        block = block.reshape(5, 5, 8, 128)
        eo = even_odd([block[:, i] for i in range(5)])
        tl, tr = line_traces(eo)
        out = line_apply(
            eo,
            pick(first_lane, -tl, lanes_roll(tr, 1)),
            pick(last_lane, -tr, lanes_roll(tl, -1)),
        )
        for b in range(5):
            r[v, pl.ds(25 * a + 5 * b, 5)] = jnp.stack([out[i][b] for i in range(5)])
        return carry

    lax.fori_loop(0, 25, normal_part, 0)

    end_lo = jnp.logical_and(row_lo, jnp.logical_not(has_lo))
    end_hi = jnp.logical_and(row_hi, jnp.logical_not(has_hi))

    def unpack(from_left, from_right, dst, first, count, step):
        def body(k, carry):
            p = first + step * k
            a, b = from_left[pl.ds(p, step)], from_right[pl.ds(p, step)]
            one = pick(low_j, a, rows_roll(b, 1))
            other = pick(low_j, rows_roll(a, -1), b)
            dst[pl.ds(2 * p, 2 * step)] = jnp.stack([one, other], axis=1).reshape(
                2 * step, 8, 128
            )
            return carry

        lax.fori_loop(0, count // step, body, 0)

    def chord_outer(from_lo, from_hi, q):
        lo = from_lo[pl.ds(PAD + q, 5)]
        hi = from_hi[pl.ds(PAD + q, 5)]
        gap = jnp.zeros((5, 4, 128), jnp.float32)
        return jnp.concatenate([lo, gap, hi], axis=1)

    def span_part(k, carry):
        v = k // 5
        a = k - 5 * v
        outer = tsf[pl.ds(25 * v + 5 * a, 5)]
        flux = [
            vis[pl.ds(25 * a + 5 * b, 5)]
            * (gs[v, pl.ds(25 * a + 5 * b, 5)] + span_lift[b][None] * outer)
            for b in range(5)
        ]
        eo = even_odd(flux)
        tl, tr = line_traces(eo)
        zero = jnp.zeros_like(tl)
        out = line_apply(
            eo, pick(low_j, zero, rows_roll(tr, 1)), pick(low_j, rows_roll(tl, -1), zero)
        )
        for b in range(5):
            at = pl.ds(25 * a + 5 * b, 5)
            r[v, at] = r[v, at] + out[b]
        return carry

    def chord_part(k, carry):
        v = k // 5
        b = k - 5 * v
        q = 25 * v + 5 * b
        own = tc[pl.ds(q, 5)]
        outer = chord_outer(vcu, vcd, q)
        outer = pick(jnp.logical_or(end_lo, end_hi), own, outer)
        flux = [
            vis[pl.ds(25 * a + 5 * b, 5)]
            * (gc[v, pl.ds(25 * a + 5 * b, 5)] + chord_lift[a][None] * outer)
            for a in range(5)
        ]
        eo = even_odd(flux)
        tl, tr = line_traces(eo)
        zero = jnp.zeros_like(tl)
        out = line_apply(
            eo,
            pick(row_lo, pick(end_lo, -tl, zero), rows_roll(tr, 2)),
            pick(row_hi, pick(end_hi, -tr, zero), rows_roll(tl, -2)),
        )
        for a in range(5):
            at = pl.ds(25 * a + 5 * b, 5)
            r[v, at] = r[v, at] + out[a]
        return carry

    for g, (v0, v1) in enumerate(GROUPS):
        arrive(u_copies[g])
        count = -(-25 * (v1 - v0) // 2)
        unpack(vsr, vsl, tsf, 25 * v0 // 2, count, 5 if count % 5 == 0 else count)
        lax.fori_loop(5 * v0, 5 * v1, span_part, 0)
        lax.fori_loop(5 * v0, 5 * v1, chord_part, 0)
        pass_on(f_copies[g])

    def span_outer(q, at):
        return tsf[pl.ds(q, 5)] + ks[pl.ds(at, 5)] * ts[pl.ds(q, 5)]

    def chord_flux(q, at):
        outer = chord_outer(hcu, hcd, q) + kc[pl.ds(at, 5)] * tc[pl.ds(q, 5)]
        return pick(jnp.logical_or(end_lo, end_hi), jnp.zeros_like(outer), outer)

    def finish(k, carry):
        v = k // 5
        a = k - 5 * v
        outer = span_outer(25 * v + 5 * a, 5 * a)
        for b in range(5):
            at = pl.ds(25 * a + 5 * b, 5)
            r[v, at] = r[v, at] + span_lift[b][None] * outer
        return carry

    def finish_chord(k, carry):
        v = k // 5
        b = k - 5 * v
        outer = chord_flux(25 * v + 5 * b, 5 * b)
        for a in range(5):
            at = pl.ds(25 * a + 5 * b, 5)
            r[v, at] = r[v, at] + chord_lift[a][None] * outer
        return carry

    for g, (v0, v1) in enumerate(GROUPS):
        arrive(f_copies[g])
        count = -(-25 * (v1 - v0) // 2)
        unpack(hsr, hsl, tsf, 25 * v0 // 2, count, 5 if count % 5 == 0 else count)
        if g < 2:
            lax.fori_loop(5 * v0, 5 * v1, finish, 0)
            lax.fori_loop(5 * v0, 5 * v1, finish_chord, 0)
        else:
            for k in range(5):
                at = pl.ds(5 * k, 5)
                out_s[at] = span_outer(100 + 5 * k, 5 * k)
                out_c[at] = chord_flux(100 + 5 * k, 5 * k)
    for dc, ds, copy in eps_copies:
        guarded(exists(dc), copy.wait_send)
    for g in range(3):
        sent(u_copies[g])
        sent(f_copies[g])


def store_kernel(r, vis, out_s, out_c, res_hbm, vis_hbm, final, sem):
    copies = [pltpu.make_async_copy(r.at[v], res_hbm.at[v], sem.at[v]) for v in range(4)]
    copies.append(pltpu.make_async_copy(vis, vis_hbm, sem.at[5]))
    for copy in copies:
        copy.start()
    span, chord = lift_rows()
    for a in range(5):
        for b in range(5):
            at = pl.ds(25 * a + 5 * b, 5)
            final[at] = (
                r[4, at]
                + span[b][None] * out_s[pl.ds(5 * a, 5)]
                + chord[a][None] * out_c[pl.ds(5 * b, 5)]
            )
    copies.append(pltpu.make_async_copy(final, res_hbm.at[4], sem.at[4]))
    copies[-1].start()
    for copy in copies:
        copy.wait()


def shards(state):
    chords, spans = lax.axis_size("chord"), lax.axis_size("span")
    f32 = jnp.float32
    field = pltpu.VMEM((5, 125, 8, 128), f32)
    pairs = pltpu.VMEM((PAIRS, 8, 128), f32)
    thin = pltpu.VMEM((125 + 2 * PAD, 2, 128), f32)
    sem = pltpu.SemaphoreType.DMA
    partial, viscosity, out_s, out_c = pl.pallas_call(
        functools.partial(kernel, chords, spans),
        out_shape=(
            jax.ShapeDtypeStruct((5, 125, 8, 128), f32),
            jax.ShapeDtypeStruct((125, 8, 128), f32),
            jax.ShapeDtypeStruct((25, 8, 128), f32),
            jax.ShapeDtypeStruct((25, 8, 128), f32),
        ),
        in_specs=[pl.BlockSpec(memory_space=pltpu.HBM)],
        out_specs=(pl.BlockSpec(memory_space=pltpu.VMEM),) * 4,
        scratch_shapes=[
            field,
            field,
            field,
            field,
            pltpu.VMEM((125, 8, 128), f32),
            pltpu.VMEM((126, 8, 128), f32),
            pltpu.VMEM((125, 8, 128), f32),
            pltpu.VMEM((126, 8, 128), f32),
        ]
        + [pairs, pairs, thin, thin] * 4
        + [thin]
        + [
            pltpu.VMEM((8, 128), f32),
            pltpu.VMEM((8, 8, 128), f32),
            pltpu.VMEM((25, 8, 128), f32),
            pltpu.VMEM((25, 8, 128), f32),
            sem((5,)),
            sem((8,)),
            sem((8,)),
            sem((12,)),
            sem((12,)),
            sem((12,)),
            sem((12,)),
            sem((len(RELAYS),)),
            sem((len(RELAYS),)),
        ],
        compiler_params=pltpu.CompilerParams(
            collective_id=0, has_side_effects=True, vmem_limit_bytes=40 * 1024 * 1024
        ),
        name="viscous",
    )(pltpu.with_memory_space_constraint(state.reshape(5, 125, 8, 128), pltpu.HBM))
    residual, viscosity = pl.pallas_call(
        store_kernel,
        out_shape=(
            jax.ShapeDtypeStruct((5, 125, 8, 128), f32),
            jax.ShapeDtypeStruct((125, 8, 128), f32),
        ),
        in_specs=[pl.BlockSpec(memory_space=pltpu.VMEM)] * 4,
        out_specs=(pl.BlockSpec(memory_space=pl.ANY), pl.BlockSpec(memory_space=pl.ANY)),
        scratch_shapes=[pltpu.VMEM((125, 8, 128), f32), sem((6,))],
        compiler_params=pltpu.CompilerParams(vmem_limit_bytes=4 * 1024 * 1024),
        name="store",
    )(partial, viscosity, out_s, out_c)
    return residual.reshape(state.shape), viscosity.reshape(state.shape[1:])


def solution(mesh):
    in_specs = (P(None, None, "chord", "span", None),)
    out_specs = (P(None, None, "chord", "span", None), P(None, "chord", "span", None))
    return jax.shard_map(shards, mesh=mesh, in_specs=in_specs, out_specs=out_specs, check_vma=False)
```
